32 devices in a mesh: seq: 8 (over z, x), head: 4 (over y, core).
Axes of the slice: x: 2, y: 2, z: 4, core: 2. Of those that a mesh axis runs over, the one named last changes fastest.
Arguments:
- prompt_queries: bfloat16 [1536, 4096], P('seq', 'head'), may hold values from -16 to 16
- prompt_keys: bfloat16 [1536, 1024], P('seq', 'head'), may hold values from -16 to 16
- prompt_values: bfloat16 [1536, 1024], P('seq', 'head'), may hold values from -6 to 6
- span_offset: int32 [8], P('seq'), may hold values from 0 to 7, each once
- appended_queries: bfloat16 [8, 4096], P(None, 'head'), may hold values from -16 to 16
- appended_keys: bfloat16 [8, 1024], P(None, 'head'), may hold values from -6 to 6
- appended_values: bfloat16 [8, 1024], P(None, 'head'), may hold values from -6 to 6
- dec_pos: int32 [8], replicated, may hold values from 2 to 1536, as said below
- out_weight: bfloat16 [4096, 4096], P('head'), may hold values from -0.09375 to 0.09375
Outputs:
- layer_out: bfloat16 [1536, 4096], P(('seq', 'head'))
- dec_out: bfloat16 [8, 4096], P('seq', 'head')
The draws below stay inside these ranges and needn't reach their ends.
Inputs may be any that keep to these rules, and one draw needn't show every extreme that they name: span_offset is a permutation of 0 to 7. `dec_pos`: some appended token stands at 1536 in every draw.
All inputs are finite; a program needn't handle non-finite values.
Results may differ from the reference program's by a relative error of at most 0.015.
Values may be sent and summed in bfloat16 or wider, within the bound.
A program may use at most 256 MiB of HBM per device.

```python
import math
import jax
import jax.numpy as jnp
from jax import lax

D = 4096
QUERY_HEADS = 32
KEY_VALUE_HEADS = 8
HEAD_SIZE = 128
TOK_DEV = 192
PROMPT_TOKENS = 1536
APPENDED_TOKENS = 8
N_SEQ = 8


def offset_values(key, shape):
    return jnp.clip(jax.random.normal(key, shape, jnp.float32), -6.0, 6.0)


def draw_prompt_queries(key, part):
    base_offset = offset_values(jax.random.fold_in(key, 1), (PROMPT_TOKENS, QUERY_HEADS, HEAD_SIZE))
    return base_offset.reshape(PROMPT_TOKENS, QUERY_HEADS * HEAD_SIZE).astype(jnp.bfloat16)


def draw_prompt_keys(key, part):
    base_offset = offset_values(jax.random.fold_in(key, 2), (PROMPT_TOKENS, KEY_VALUE_HEADS, HEAD_SIZE))
    return base_offset.reshape(PROMPT_TOKENS, KEY_VALUE_HEADS * HEAD_SIZE).astype(jnp.bfloat16)


def draw_appended_queries(key, part):
    base_offset = offset_values(jax.random.fold_in(key, 3), (APPENDED_TOKENS, QUERY_HEADS, HEAD_SIZE))
    return base_offset.reshape(APPENDED_TOKENS, QUERY_HEADS * HEAD_SIZE).astype(jnp.bfloat16)


def draw_dec_pos(key, part):
    top_bit = max(PROMPT_TOKENS.bit_length() - 1, 1)
    powers = jax.random.randint(jax.random.fold_in(key, 4), (APPENDED_TOKENS,), 1, top_bit + 1)
    lowest = jnp.left_shift(jnp.ones((APPENDED_TOKENS,), jnp.int32), powers.astype(jnp.int32))
    extra = jax.random.randint(jax.random.fold_in(key, 5), (APPENDED_TOKENS,), 0, lowest)
    placed = jnp.minimum(lowest + extra, PROMPT_TOKENS)
    row_ids = jnp.arange(APPENDED_TOKENS, dtype=jnp.int32)
    return jnp.where(row_ids == 0, PROMPT_TOKENS, placed).astype(jnp.int32)


def level_of(rng, dims, shards, least, high):
    factor_of = 1.0
    for dim, blocks in shards:
        heights = jax.random.uniform(jax.random.fold_in(jax.random.fold_in(rng, 6), dim), (blocks,), jnp.float32, least / len(shards), high / len(shards))
        factor_of = factor_of * jnp.repeat(jnp.exp(heights), dims[dim] // blocks).reshape((-1,) + (1,) * (len(dims) - 1 - dim))
    return factor_of


def centred(rng, extent, spread, limit, cuts=(), kind=jnp.bfloat16):
    array = jax.random.normal(rng, extent, jnp.float32) * spread
    if len(cuts) > 0:
        array = level_of(rng, extent, cuts, -0.22, 0.18) * array
    return jnp.clip(array, min=-limit, max=limit).astype(kind)


def setup_inputs(seed: int = 0) -> dict:
    arg_keys = jax.random.split(jax.random.key(seed), 10)
    prompt_queries = draw_prompt_queries(jax.random.fold_in(arg_keys[9], 71), 0)
    prompt_keys = draw_prompt_keys(jax.random.fold_in(arg_keys[9], 71), 0)
    prompt_values = centred(arg_keys[2], (PROMPT_TOKENS, KEY_VALUE_HEADS * HEAD_SIZE), 1.0, 6.0, ((0, 8), (1, 4)))
    span_offset = jax.random.permutation(arg_keys[3], N_SEQ).astype(jnp.int32)
    appended_queries = draw_appended_queries(jax.random.fold_in(arg_keys[9], 71), 0)
    appended_keys = centred(arg_keys[5], (APPENDED_TOKENS, KEY_VALUE_HEADS * HEAD_SIZE), 1.0, 6.0, ((1, 4),))
    appended_values = centred(arg_keys[6], (APPENDED_TOKENS, KEY_VALUE_HEADS * HEAD_SIZE), 1.0, 6.0, ((1, 4),))
    dec_pos = draw_dec_pos(jax.random.fold_in(arg_keys[9], 71), 0)
    out_weight = centred(arg_keys[8], (QUERY_HEADS * HEAD_SIZE, D), (QUERY_HEADS * HEAD_SIZE) ** -0.5, 0.09375, ((0, 4),))
    return {"prompt_queries": prompt_queries, "prompt_keys": prompt_keys, "prompt_values": prompt_values, "span_offset": span_offset, "appended_queries": appended_queries, "appended_keys": appended_keys, "appended_values": appended_values, "dec_pos": dec_pos, "out_weight": out_weight}


masked_score = -1e30


def round_trip(values):
    return lax.optimization_barrier(values.astype(jnp.bfloat16)).astype(jnp.float32)


def reference(prompt_queries, prompt_keys, prompt_values, span_offset, appended_queries, appended_keys, appended_values, dec_pos, out_weight):
    group_width = QUERY_HEADS // KEY_VALUE_HEADS
    score_scale = HEAD_SIZE ** -0.5
    slots = jnp.arange(N_SEQ, dtype=jnp.int32)
    inverse = jnp.sum(slots[:, None] * (span_offset[:, None] == slots[None, :]).astype(jnp.int32), axis=0)

    def order_rows(matrix):
        return matrix.reshape(N_SEQ, TOK_DEV, matrix.shape[1])[inverse].reshape(PROMPT_TOKENS, matrix.shape[1])

    queries_ordered = order_rows(prompt_queries).reshape(PROMPT_TOKENS, KEY_VALUE_HEADS, group_width, HEAD_SIZE).transpose(1, 0, 2, 3).astype(jnp.float32)
    keys_ordered = order_rows(prompt_keys).reshape(PROMPT_TOKENS, KEY_VALUE_HEADS, HEAD_SIZE).transpose(1, 0, 2).astype(jnp.float32)
    values_ordered = order_rows(prompt_values).reshape(PROMPT_TOKENS, KEY_VALUE_HEADS, HEAD_SIZE).transpose(1, 0, 2).astype(jnp.float32)
    query_gradient_full = appended_queries.reshape(APPENDED_TOKENS, KEY_VALUE_HEADS, group_width, HEAD_SIZE).transpose(1, 0, 2, 3).astype(jnp.float32)
    key_gradient_full = appended_keys.reshape(APPENDED_TOKENS, KEY_VALUE_HEADS, HEAD_SIZE).transpose(1, 0, 2).astype(jnp.float32)
    value_gradient_full = appended_values.reshape(APPENDED_TOKENS, KEY_VALUE_HEADS, HEAD_SIZE).transpose(1, 0, 2).astype(jnp.float32)
    block = math.gcd(PROMPT_TOKENS, 512)
    positions = jnp.arange(PROMPT_TOKENS, dtype=jnp.int32)

    def one_group(operands):
        q_rows, k_rows, v_rows, dq_rows, dk_rows, dv_rows = operands
        pieces = []
        for number in range(PROMPT_TOKENS // block):
            begin = number * block
            finish = begin + block
            scores = jnp.einsum("rgd,sd->rgs", q_rows[begin:finish], k_rows[:finish]) * score_scale
            allowed = (positions[None, :finish] <= positions[begin:finish, None])[:, None, :]
            row_max = jnp.max(jnp.where(allowed, scores, masked_score), axis=-1, keepdims=True)
            weights = jnp.where(allowed, jnp.exp(scores - row_max), 0.0)
            denominator = jnp.sum(weights, axis=-1, keepdims=True)
            summed = jnp.einsum("rgs,sd->rgd", round_trip(weights), v_rows[:finish])
            pieces.append((summed / denominator).astype(jnp.bfloat16))
        dec_scores = jnp.einsum("rgd,sd->rgs", dq_rows, k_rows) * score_scale
        visible = (positions[None, :] < dec_pos[:, None])[:, None, :]
        self_score = jnp.einsum("rgd,rd->rg", dq_rows, dk_rows) * score_scale
        dec_max = jnp.maximum(jnp.max(jnp.where(visible, dec_scores, masked_score), axis=-1), self_score)
        dec_weights = jnp.where(visible, jnp.exp(dec_scores - dec_max[..., None]), 0.0)
        self_weight = jnp.exp(self_score - dec_max)
        dec_denominator = jnp.sum(dec_weights, axis=-1) + self_weight
        dec_summed = jnp.einsum("rgs,sd->rgd", round_trip(dec_weights), v_rows)
        dec_summed = dec_summed + round_trip(self_weight)[..., None] * dv_rows[:, None, :]
        dec_piece = (dec_summed / dec_denominator[..., None]).astype(jnp.bfloat16)
        return jnp.concatenate(pieces, axis=0), dec_piece

    prompt_attn, dec_attn = lax.map(one_group, (queries_ordered, keys_ordered, values_ordered, query_gradient_full, key_gradient_full, value_gradient_full))
    attn_sorted = prompt_attn.transpose(1, 0, 2, 3).reshape(PROMPT_TOKENS, QUERY_HEADS * HEAD_SIZE)
    attention = attn_sorted.reshape(N_SEQ, TOK_DEV, QUERY_HEADS * HEAD_SIZE)[span_offset].reshape(PROMPT_TOKENS, QUERY_HEADS * HEAD_SIZE)
    layer_out = jnp.dot(attention, out_weight, preferred_element_type=jnp.float32).astype(jnp.bfloat16)
    dec_attention = dec_attn.transpose(1, 0, 2, 3).reshape(APPENDED_TOKENS, QUERY_HEADS * HEAD_SIZE)
    dec_out = jnp.dot(dec_attention, out_weight, preferred_element_type=jnp.float32).astype(jnp.bfloat16)
    return layer_out, dec_out
```

```python
import functools
import math

import jax
import jax.numpy as jnp
from jax import lax
from jax.experimental import pallas as pl
from jax.experimental.pallas import tpu as pltpu
from jax.sharding import PartitionSpec as P

QUERY_HEADS = 32
KEY_VALUE_HEADS = 8
HEAD_SIZE = 128
GROUP = QUERY_HEADS // KEY_VALUE_HEADS
MESH = pl.DeviceIdType.MESH
LANES = 128
MARK = 16

masked_score = -1e30
exp2_scale = HEAD_SIZE ** (-0.5) * math.log2(math.e)
LEFT, RIGHT, SIDE = 0, 1, 2


def hand_on(layer_in, dec_in, layer_out, dec_out):
    layer_out[...] = layer_in[...]
    dec_out[...] = dec_in[0 : dec_out.shape[0]].astype(dec_out.dtype)


def in_hbm(array):
    return pltpu.with_memory_space_constraint(array, pltpu.MemorySpace.HBM)


def both(*conditions):
    result = conditions[0]
    for condition in conditions[1:]:
        result = jnp.logical_and(result, condition)
    return result


def kernel(
    n_seq, own_dec, chunk, n_dec, tok,
    q_hbm, k_hbm, v_hbm, span_ref, aq_hbm, ak_hbm, av_hbm, pos_hbm, w_hbm,
    out_ref, dec_ref,
    kbuf, vbuf, wbuf, qs, aq_ref, ak_ref, av_ref, m_ref, l_ref, acc_ref,
    pos_ref, attn, pbuf, own, send1, recv1, send2, recv2, dpart, dsend, drecv,
    kv_sem, q_sem, a_sem, w_sem, ss, rs, ss1, rs1, ss2, rs2, dss, drs,
):
    kv_heads = kbuf.shape[1]
    model = w_hbm.shape[1]
    part = tok // 4
    line = n_seq // 2
    rows = GROUP * tok
    lanes = qs.shape[1]
    dec_lanes = lanes - rows
    f32, b16 = jnp.float32, jnp.bfloat16
    seq = lax.axis_index("seq")
    head = lax.axis_index("head")
    z, x = seq // 2, seq % 2
    y, c = head // 2, head % 2
    partner = 2 * z + 1 - x
    to_x = (partner, head)
    to_right = (jnp.minimum(seq + 2, n_seq - 1), head)
    to_left = (jnp.maximum(seq - 2, 0), head)
    to_core = (seq, 2 * y + 1 - c)
    to_y = (seq, 2 * (1 - y) + c)
    to_diag = (seq, 2 * (1 - y) + 1 - c)
    has_left, has_right = z > 0, z < line - 1
    targets = (to_left, to_right, to_x)

    pieces = [(h, kind) for h in range(kv_heads) for kind in (0, 1)]
    early_head = kv_heads - 1

    def column(ref, i):
        return ref.at[:, pl.ds(i * HEAD_SIZE, HEAD_SIZE)]

    kv_copies = []
    for p, (h, kind) in enumerate(pieces):
        source, buffer = ((k_hbm, kbuf), (v_hbm, vbuf))[kind]
        kv_copies.append(pltpu.make_async_copy(
            column(source, h), buffer.at[seq, h, pl.ds(0, tok)], kv_sem.at[p]
        ))
        kv_copies[-1].start()
    small_copies = [
        pltpu.make_async_copy(source, buffer, a_sem.at[i])
        for i, (source, buffer) in enumerate(
            (
                (pos_hbm, pos_ref), (aq_hbm, aq_ref),
                (ak_hbm, ak_ref), (av_hbm, av_ref),
            )
        )
    ]
    for copy in small_copies:
        copy.start()
    q_copies = []
    for h in range(kv_heads):
        for g in range(GROUP):
            i = h * GROUP + g
            q_copies.append(pltpu.make_async_copy(
                column(q_hbm, i), qs.at[h, pl.ds(g * tok, tok)], q_sem.at[i]
            ))
            q_copies[-1].start()
    weight_copy = pltpu.make_async_copy(w_hbm, wbuf, w_sem)
    weight_copy.start()

    barrier = pltpu.get_barrier_semaphore()
    for peer in (to_x, to_core, to_y, to_diag):
        pl.semaphore_signal(barrier, inc=1, device_id=peer, device_id_type=MESH)
    pl.when(has_left)(
        lambda: pl.semaphore_signal(barrier, inc=1, device_id=to_left, device_id_type=MESH)
    )
    pl.when(has_right)(
        lambda: pl.semaphore_signal(barrier, inc=1, device_id=to_right, device_id_type=MESH)
    )
    own_mark = jnp.full((MARK, LANES), span_ref[0], jnp.int32).astype(f32)
    kbuf[seq, 0, pl.ds(tok, MARK), :] = own_mark.astype(b16)
    own_off = own_mark[0:1, 0:1]
    pl.semaphore_wait(barrier, 4 + jnp.where(has_left, 1, 0) + jnp.where(has_right, 1, 0))

    def moved(p, origin, way):
        h, kind = pieces[p]
        count = tok + MARK if p == 0 else tok
        slot = (kbuf, vbuf)[kind].at[origin, h, pl.ds(0, count)]
        return pltpu.make_async_remote_copy(
            src_ref=slot, dst_ref=slot,
            send_sem=ss.at[way, p, origin], recv_sem=rs.at[p, origin],
            device_id=targets[way], device_id_type=MESH,
        )

    def early(p):
        return pieces[p][0] == early_head

    for p in range(len(pieces)):
        kv_copies[p].wait()
        moved(p, seq, SIDE).start()
        pl.when(has_left)(lambda: moved(p, seq, LEFT).start())
        pl.when(has_right)(lambda: moved(p, seq, RIGHT).start())

    def relay_own(d, p):
        @pl.when(z >= d)
        def _():
            origin = 2 * (z - d) + x
            moved(p, origin, RIGHT).wait_recv()
            pl.when(has_right)(lambda: moved(p, origin, RIGHT).start())
            if early(p):
                pl.when(z != d)(lambda: moved(p, origin, SIDE).start())
            else:
                moved(p, origin, SIDE).start()

        @pl.when(z + d < line)
        def _():
            origin = 2 * (z + d) + x
            moved(p, origin, LEFT).wait_recv()
            pl.when(has_left)(lambda: moved(p, origin, LEFT).start())
            if early(p):
                pl.when(z + d != line - 1)(lambda: moved(p, origin, SIDE).start())
            else:
                moved(p, origin, SIDE).start()

    def relay_partner(p):
        moved(p, partner, SIDE).wait_recv()
        if early(p):
            pl.when(z == 0)(lambda: moved(p, partner, RIGHT).start())
            pl.when(z == line - 1)(lambda: moved(p, partner, LEFT).start())

    def relay_corner(d, p):
        @pl.when(z == d)
        def _():
            moved(p, 1 - x, RIGHT).wait_recv()
            pl.when(has_right)(lambda: moved(p, 1 - x, RIGHT).start())

        @pl.when(z + d == line - 1)
        def _():
            origin = 2 * (line - 1) + 1 - x
            moved(p, origin, LEFT).wait_recv()
            pl.when(has_left)(lambda: moved(p, origin, LEFT).start())

    key_id = lax.broadcasted_iota(jnp.int32, (tok, 1), 0).astype(f32)
    dec_lane = lax.broadcasted_iota(jnp.int32, (1, dec_lanes), 1)
    small_copies[0].wait()
    dec_limit = jnp.zeros((1, dec_lanes), jnp.int32)
    for i in range(n_dec):
        dec_limit = jnp.where(
            jnp.logical_and(dec_lane % n_dec == i, dec_lane < GROUP * n_dec), pos_ref[i], dec_limit
        )
    dec_limit = dec_limit.astype(f32)
    query_row = (lax.broadcasted_iota(jnp.int32, (1, rows), 1) % tok).astype(f32)

    def weigh(block, h, diagonal=False):
        offset = own_off if diagonal else kbuf[block, 0, pl.ds(tok, MARK), :][0:1, 0:1].astype(f32)
        scores = lax.dot_general(
            kbuf[block, h, pl.ds(0, tok), :], qs[h], (((1,), (1,)), ((), ())),
            preferred_element_type=f32,
        )
        dec_seen = offset * tok + key_id < dec_limit
        dec_scores = jnp.where(dec_seen, scores[:, rows:], masked_score)
        scores = scores[:, :rows]
        if diagonal:
            scores = jnp.where(key_id <= query_row, scores, masked_score)
        old = m_ref[h][0:1]
        top = jnp.max(scores, axis=0, keepdims=True)
        new = jnp.maximum(old[:, :rows], top)
        if diagonal:
            used = new
        else:
            seen = offset <= own_off
            new = jnp.where(seen, new, old[:, :rows])
            used = jnp.where(seen, new, -masked_score)
        dec_new = jnp.maximum(old[:, rows:], jnp.max(dec_scores, axis=0, keepdims=True))
        new = jnp.concatenate([new, dec_new], axis=1)
        weights = jnp.concatenate([
            jnp.exp2((scores - used) * exp2_scale),
            jnp.exp2((dec_scores - dec_new) * exp2_scale),
        ], axis=1)
        factor = jnp.exp2((old - new) * exp2_scale)
        m_ref[h] = jnp.broadcast_to(new, m_ref.shape[1:])
        l_ref[h] = l_ref[h] * factor + jnp.sum(weights, axis=0, keepdims=True)
        return weights.astype(b16), factor

    def gather_values(block, h, weights, factor):
        added = lax.dot_general(
            vbuf[block, h], weights, (((0,), (0,)), ((), ())), preferred_element_type=f32
        )
        acc_ref[h] = acc_ref[h] * factor + added

    def attend(block, h, diagonal=False):
        weights, factor = weigh(block, h, diagonal)
        gather_values(block, h, weights, factor)

    for copy in small_copies[1:]:
        copy.wait()
    pad = dec_lanes - GROUP * n_dec
    for h in range(kv_heads):
        q32 = jnp.concatenate([
            aq_ref[:, (h * GROUP + g) * HEAD_SIZE : (h * GROUP + g + 1) * HEAD_SIZE].astype(f32)
            for g in range(GROUP)
        ] + ([jnp.zeros((pad, HEAD_SIZE), f32)] if pad else []), axis=0)
        dec_q = q32.astype(b16)
        qs[h, pl.ds(rows, dec_lanes), :] = dec_q
        cols = slice(h * HEAD_SIZE, (h + 1) * HEAD_SIZE)
        own_lane = lax.broadcasted_iota(jnp.int32, (n_dec, dec_lanes), 1)
        own_token = lax.broadcasted_iota(jnp.int32, (n_dec, dec_lanes), 0)
        mine = jnp.logical_and(own_lane % n_dec == own_token, own_lane < GROUP * n_dec)
        pair_scores = lax.dot_general(
            ak_ref[:, cols], dec_q, (((1,), (1,)), ((), ())), preferred_element_type=f32
        )
        self_score = jnp.sum(jnp.where(mine, pair_scores, 0.0), axis=0, keepdims=True)
        picked = lax.dot_general(
            av_ref[:, cols].astype(f32), mine.astype(f32), (((0,), (0,)), ((), ())),
            preferred_element_type=f32,
        )
        m_ref[h] = jnp.broadcast_to(
            jnp.concatenate([jnp.full((1, rows), masked_score, f32), self_score], axis=1),
            m_ref.shape[1:],
        )
        l_ref[h] = jnp.concatenate(
            [jnp.zeros((8, rows), f32), jnp.ones((8, dec_lanes), f32)], axis=1
        )
        acc_ref[h] = jnp.concatenate([jnp.zeros((HEAD_SIZE, rows), f32), picked], axis=1)
    for h in range(kv_heads):
        for g in range(GROUP):
            q_copies[h * GROUP + g].wait()
        attend(seq, h, diagonal=True)

    def near(d, h):
        pl.when(z >= d)(lambda: attend(2 * (z - d) + x, h))
        pl.when(z + d < line)(lambda: attend(2 * (z + d) + x, h))

    def await_side(d, h):
        for p in (2 * h, 2 * h + 1):
            if h == early_head:
                pl.when(z > d)(lambda: moved(p, 2 * (z - d) + 1 - x, SIDE).wait_recv())
                pl.when(z + d < line - 1)(
                    lambda: moved(p, 2 * (z + d) + 1 - x, SIDE).wait_recv()
                )
            else:
                pl.when(z >= d)(lambda: moved(p, 2 * (z - d) + 1 - x, SIDE).wait_recv())
                pl.when(z + d < line)(lambda: moved(p, 2 * (z + d) + 1 - x, SIDE).wait_recv())

    def across(d, h):
        await_side(d, h)
        pl.when(z >= d)(lambda: attend(2 * (z - d) + 1 - x, h))
        pl.when(z + d < line)(lambda: attend(2 * (z + d) + 1 - x, h))

    corner_k, corner_v = 2 * early_head, 2 * early_head + 1

    for p, (h, kind) in enumerate(pieces):
        relay_own(1, p)
        relay_partner(p)
        if kind == 1:
            near(1, h)
    for h in range(kv_heads - 1):
        attend(partner, h)

    def round_(r, carry):
        for p, (h, kind) in enumerate(pieces):
            relay_own(r, p)
            if p == 1:
                relay_corner(r - 1, corner_k)
            if p == 2:
                relay_corner(r - 1, corner_v)
            if kind == 1:
                near(r, h)
                if p == 1:
                    @pl.when(r == 2)
                    def _():
                        attend(partner, early_head)

                    @pl.when(r > 2)
                    def _():
                        across(r - 2, early_head)
        for h in range(kv_heads - 1):
            across(r - 1, h)
        return carry

    lax.fori_loop(2, line, round_, 0)
    across(line - 2, early_head)
    relay_corner(line - 1, corner_k)
    relay_corner(line - 1, corner_v)
    for h in range(kv_heads - 1):
        await_side(line - 1, h)
    for h in range(kv_heads):
        pl.when(z >= line - 1)(lambda: attend(1 - x, h))
        pl.when(z < 1)(lambda: attend(2 * (line - 1) + 1 - x, h))

    dec_pad = attn.shape[0] - tok - n_dec
    for h in range(kv_heads):
        turned = jnp.transpose(acc_ref[h] * (1.0 / l_ref[h][0:1]))
        for g in range(GROUP):
            i = h * GROUP + g
            cols = slice(i * HEAD_SIZE, (i + 1) * HEAD_SIZE)
            attn[0:tok, cols] = turned[g * tok : (g + 1) * tok].astype(b16)
            dec = turned[rows + g * n_dec : rows + (g + 1) * n_dec]
            if dec_pad:
                dec = jnp.concatenate([dec, jnp.zeros((dec_pad, HEAD_SIZE), f32)], axis=0)
            attn[tok:, cols] = dec.astype(b16)
    weight_copy.wait()

    n_chunk = model // chunk

    def core_copy(i):
        return pltpu.make_async_remote_copy(
            src_ref=send1.at[i], dst_ref=recv1.at[i], send_sem=ss1.at[i], recv_sem=rs1.at[i],
            device_id=to_core, device_id_type=MESH,
        )

    def y_copy(i):
        return pltpu.make_async_remote_copy(
            src_ref=send2.at[i], dst_ref=recv2.at[i], send_sem=ss2.at[i], recv_sem=rs2.at[i],
            device_id=to_y, device_id_type=MESH,
        )

    def block(index):
        return pl.ds(pl.multiple_of(index * part, 8), part)

    def project(i, carry):
        @pl.when(i < n_chunk)
        def _():
            cols = pl.ds(pl.multiple_of(i * chunk, chunk), chunk)
            pbuf[...] = jnp.dot(attn[...], wbuf[:, cols], preferred_element_type=f32)
            send1[i, 0:part] = pbuf[block(2 * (1 - y) + 1 - c)].astype(b16)
            send1[i, part:] = pbuf[block(2 * y + 1 - c)].astype(b16)
            core_copy(i).start()
            own[i, 0:part] = pbuf[block(2 * (1 - y) + c)]
            own[i, part:] = pbuf[block(2 * y + c)]
            dpart[:, cols] = pbuf[tok : tok + n_dec]

        @pl.when(i > 0)
        def _():
            core_copy(i - 1).wait_recv()
            total = own[i - 1, 0:part] + recv1[i - 1, 0:part].astype(f32)
            send2[i - 1] = total.astype(b16)
            y_copy(i - 1).start()

        return carry

    lax.fori_loop(0, n_chunk + 1, project, 0)

    quarter = model // 4
    mine = pl.ds(seq * own_dec, own_dec)

    def dec_copy(way, peer):
        return pltpu.make_async_remote_copy(
            src_ref=dsend.at[way], dst_ref=drecv.at[way],
            send_sem=dss.at[way], recv_sem=drs.at[way],
            device_id=peer, device_id_type=MESH,
        )

    dec_copies = []
    for way, peer in enumerate((to_core, to_y, to_diag)):
        cols = pl.ds(pl.multiple_of(peer[1] * quarter, 128), quarter)
        dsend[way] = dpart[mine, cols]
        dec_copies.append(dec_copy(way, peer))
        dec_copies[-1].start()

    def gather_sum(i, carry):
        y_copy(i).wait_recv()
        cols = pl.ds(pl.multiple_of(i * chunk, chunk), chunk)
        total = own[i, part:] + recv1[i, part:].astype(f32)
        out_ref[:, cols] = (total + recv2[i].astype(f32)).astype(b16)
        y_copy(i).wait_send()
        core_copy(i).wait_send()
        return carry

    lax.fori_loop(0, n_chunk, gather_sum, 0)
    for copy in dec_copies:
        copy.wait()
    dec_total = dpart[mine, pl.ds(pl.multiple_of(head * quarter, 128), quarter)]
    dec_total = dec_total + drecv[0] + drecv[1] + drecv[2]
    dec_ref[...] = jnp.broadcast_to(dec_total, dec_ref.shape)

    def drain(oz, carry):
        origin = 2 * oz + x
        edge = jnp.logical_or(oz == 0, oz == line - 1)
        for p in range(len(pieces)):
            pl.when(both(oz <= z, has_right))(lambda: moved(p, origin, RIGHT).wait_send())
            pl.when(both(oz >= z, has_left))(lambda: moved(p, origin, LEFT).wait_send())
            if early(p):
                pl.when(jnp.logical_or(oz == z, jnp.logical_not(edge)))(
                    lambda: moved(p, origin, SIDE).wait_send()
                )
            else:
                moved(p, origin, SIDE).wait_send()
        return carry

    lax.fori_loop(0, line, drain, 0)
    for p in (corner_k, corner_v):
        pl.when(has_right)(lambda: moved(p, 1 - x, RIGHT).wait_send())
        pl.when(has_left)(lambda: moved(p, 2 * (line - 1) + 1 - x, LEFT).wait_send())


def on_device(
    prompt_queries, prompt_keys, prompt_values, span_offset,
    appended_queries, appended_keys, appended_values, dec_pos, out_weight,
):
    n_seq = lax.axis_size("seq")
    tok, width = prompt_queries.shape
    kv_width = prompt_keys.shape[1]
    kv_heads = kv_width // HEAD_SIZE
    heads = kv_heads * GROUP
    n_dec = appended_queries.shape[0]
    own_dec = n_dec // n_seq
    model = out_weight.shape[1]
    chunk = 512
    n_chunk = model // chunk
    part = tok // 4
    rows = tok + -(-n_dec // 16) * 16
    lanes = GROUP * tok + -(-GROUP * n_dec // LANES) * LANES
    vmem = pl.BlockSpec(memory_space=pltpu.VMEM)
    hbm = pl.BlockSpec(memory_space=pltpu.MemorySpace.HBM)
    smem = pl.BlockSpec(memory_space=pltpu.SMEM)
    f32, b16 = jnp.float32, jnp.bfloat16
    dma = pltpu.SemaphoreType.DMA
    n_piece = 2 * kv_heads
    results = pl.pallas_call(
        functools.partial(kernel, n_seq, own_dec, chunk, n_dec, tok),
        out_shape=(
            jax.ShapeDtypeStruct((part, model), b16),
            jax.ShapeDtypeStruct((8 * own_dec, model // 4), f32),
        ),
        in_specs=[hbm] * 3 + [smem] + [hbm] * 5,
        out_specs=(vmem, vmem),
        scratch_shapes=[
            pltpu.VMEM((n_seq, kv_heads, tok + MARK, HEAD_SIZE), b16),
            pltpu.VMEM((n_seq, kv_heads, tok, HEAD_SIZE), b16),
            pltpu.VMEM(out_weight.shape, b16),
            pltpu.VMEM((kv_heads, lanes, HEAD_SIZE), b16),
            pltpu.VMEM((n_dec, width), b16),
            pltpu.VMEM((n_dec, kv_width), b16),
            pltpu.VMEM((n_dec, kv_width), b16),
            pltpu.VMEM((kv_heads, 8, lanes), f32),
            pltpu.VMEM((kv_heads, 8, lanes), f32),
            pltpu.VMEM((kv_heads, HEAD_SIZE, lanes), f32),
            pltpu.SMEM((n_dec,), jnp.int32),
            pltpu.VMEM((rows, width), b16),
            pltpu.VMEM((rows, chunk), f32),
            pltpu.VMEM((n_chunk, 2 * part, chunk), f32),
            pltpu.VMEM((n_chunk, 2 * part, chunk), b16),
            pltpu.VMEM((n_chunk, 2 * part, chunk), b16),
            pltpu.VMEM((n_chunk, part, chunk), b16),
            pltpu.VMEM((n_chunk, part, chunk), b16),
            pltpu.VMEM((n_dec, model), f32),
            pltpu.VMEM((3, own_dec, model // 4), f32),
            pltpu.VMEM((3, own_dec, model // 4), f32),
            dma((n_piece,)), dma((heads,)), dma((4,)), dma,
            dma((3, n_piece, n_seq)), dma((n_piece, n_seq)),
            dma((n_chunk,)), dma((n_chunk,)), dma((n_chunk,)), dma((n_chunk,)),
            dma((3,)), dma((3,)),
        ],
        compiler_params=pltpu.CompilerParams(
            collective_id=0, has_side_effects=True, vmem_limit_bytes=44 * 2**20
        ),
    )(
        *map(in_hbm, (prompt_queries, prompt_keys, prompt_values)), span_offset,
        *map(in_hbm, (appended_queries, appended_keys, appended_values, dec_pos, out_weight)),
    )
    return pl.pallas_call(
        hand_on,
        out_shape=(
            jax.ShapeDtypeStruct((part, model), b16),
            jax.ShapeDtypeStruct((own_dec, model // 4), b16),
        ),
        in_specs=[vmem] * 2,
        out_specs=(vmem, vmem),
        compiler_params=pltpu.CompilerParams(vmem_limit_bytes=4 * 2**20),
    )(*results)


def solution(mesh):
    in_specs = (
        P("seq", "head"),
        P("seq", "head"),
        P("seq", "head"),
        P("seq"),
        P(None, "head"),
        P(None, "head"),
        P(None, "head"),
        P(),
        P("head", None),
    )
    out_specs = (P(("seq", "head"), None), P("seq", "head"))
    return jax.shard_map(
        on_device, mesh=mesh, in_specs=in_specs, out_specs=out_specs, check_vma=False
    )
```

```python
import functools
import math

import jax
import jax.numpy as jnp
from jax import lax
from jax.experimental import pallas as pl
from jax.experimental.pallas import tpu as pltpu
from jax.sharding import PartitionSpec as P

QUERY_HEADS = 32
KEY_VALUE_HEADS = 8
HEAD_SIZE = 128
GROUP = QUERY_HEADS // KEY_VALUE_HEADS
MESH = pl.DeviceIdType.MESH
LANES = 128
MARK = 16

masked_score = -1e30
exp2_scale = HEAD_SIZE ** (-0.5) * math.log2(math.e)
LEFT, RIGHT, SIDE = 0, 1, 2


def hand_on(layer_in, dec_in, layer_out, dec_out):
    layer_out[...] = layer_in[...]
    dec_out[...] = dec_in[0 : dec_out.shape[0]].astype(dec_out.dtype)


def in_hbm(array):
    return pltpu.with_memory_space_constraint(array, pltpu.MemorySpace.HBM)


def both(*conditions):
    result = conditions[0]
    for condition in conditions[1:]:
        result = jnp.logical_and(result, condition)
    return result


def kernel(
    n_seq, own_dec, chunk, n_dec, tok,
    q_hbm, k_hbm, v_hbm, span_ref, aq_hbm, ak_hbm, av_hbm, pos_hbm, w_hbm,
    out_ref, dec_ref,
    kbuf, vbuf, wbuf, qs, aq_ref, ak_ref, av_ref, m_ref, l_ref, acc_ref,
    pos_ref, attn, pbuf, own, send1, recv1, send2, recv2, dpart, dsend, drecv,
    kv_sem, q_sem, a_sem, w_sem, ss, rs, ss1, rs1, ss2, rs2, dss, drs,
):
    kv_heads = kbuf.shape[1]
    model = w_hbm.shape[1]
    part = tok // 4
    line = n_seq // 2
    rows = GROUP * tok
    lanes = qs.shape[1]
    dec_lanes = lanes - rows
    f32, b16 = jnp.float32, jnp.bfloat16
    seq = lax.axis_index("seq")
    head = lax.axis_index("head")
    z, x = seq // 2, seq % 2
    y, c = head // 2, head % 2
    partner = 2 * z + 1 - x
    to_x = (partner, head)
    to_right = (jnp.minimum(seq + 2, n_seq - 1), head)
    to_left = (jnp.maximum(seq - 2, 0), head)
    to_core = (seq, 2 * y + 1 - c)
    to_y = (seq, 2 * (1 - y) + c)
    to_diag = (seq, 2 * (1 - y) + 1 - c)
    has_left, has_right = z > 0, z < line - 1
    targets = (to_left, to_right, to_x)

    barrier = pltpu.get_barrier_semaphore()
    for peer in (to_x, to_core, to_y, to_diag):
        pl.semaphore_signal(barrier, inc=1, device_id=peer, device_id_type=MESH)
    pl.when(has_left)(
        lambda: pl.semaphore_signal(barrier, inc=1, device_id=to_left, device_id_type=MESH)
    )
    pl.when(has_right)(
        lambda: pl.semaphore_signal(barrier, inc=1, device_id=to_right, device_id_type=MESH)
    )

    pieces = [(h, kind) for h in range(kv_heads) for kind in (0, 1)]
    early_head = kv_heads - 1

    def column(ref, i):
        return ref.at[:, pl.ds(i * HEAD_SIZE, HEAD_SIZE)]

    kv_copies = []
    for p, (h, kind) in enumerate(pieces):
        source, buffer = ((k_hbm, kbuf), (v_hbm, vbuf))[kind]
        kv_copies.append(pltpu.make_async_copy(
            column(source, h), buffer.at[seq, h, pl.ds(0, tok)], kv_sem.at[p]
        ))
        kv_copies[-1].start()
    small_copies = [
        pltpu.make_async_copy(source, buffer, a_sem.at[i])
        for i, (source, buffer) in enumerate(
            (
                (pos_hbm, pos_ref), (aq_hbm, aq_ref),
                (ak_hbm, ak_ref), (av_hbm, av_ref),
            )
        )
    ]
    for copy in small_copies:
        copy.start()
    q_copies = []
    for h in range(kv_heads):
        for g in range(GROUP):
            i = h * GROUP + g
            q_copies.append(pltpu.make_async_copy(
                column(q_hbm, i), qs.at[h, pl.ds(g * tok, tok)], q_sem.at[i]
            ))
            q_copies[-1].start()
    weight_copy = pltpu.make_async_copy(w_hbm, wbuf, w_sem)
    weight_copy.start()

    own_mark = jnp.full((MARK, LANES), span_ref[0], jnp.int32).astype(f32)
    kbuf[seq, 0, pl.ds(tok, MARK), :] = own_mark.astype(b16)
    own_off = own_mark[0:1, 0:1]
    pl.semaphore_wait(barrier, 4 + jnp.where(has_left, 1, 0) + jnp.where(has_right, 1, 0))

    def moved(p, origin, way):
        h, kind = pieces[p]
        count = tok + MARK if p == 0 else tok
        slot = (kbuf, vbuf)[kind].at[origin, h, pl.ds(0, count)]
        return pltpu.make_async_remote_copy(
            src_ref=slot, dst_ref=slot,
            send_sem=ss.at[way, p, origin], recv_sem=rs.at[p, origin],
            device_id=targets[way], device_id_type=MESH,
        )

    def early(p):
        return pieces[p][0] == early_head

    for p in range(len(pieces)):
        kv_copies[p].wait()
        moved(p, seq, SIDE).start()
        pl.when(has_left)(lambda: moved(p, seq, LEFT).start())
        pl.when(has_right)(lambda: moved(p, seq, RIGHT).start())

    def relay_own(d, p):
        @pl.when(z >= d)
        def _():
            origin = 2 * (z - d) + x
            moved(p, origin, RIGHT).wait_recv()
            pl.when(has_right)(lambda: moved(p, origin, RIGHT).start())
            if early(p):
                pl.when(z != d)(lambda: moved(p, origin, SIDE).start())
            else:
                moved(p, origin, SIDE).start()

        @pl.when(z + d < line)
        def _():
            origin = 2 * (z + d) + x
            moved(p, origin, LEFT).wait_recv()
            pl.when(has_left)(lambda: moved(p, origin, LEFT).start())
            if early(p):
                pl.when(z + d != line - 1)(lambda: moved(p, origin, SIDE).start())
            else:
                moved(p, origin, SIDE).start()

    def relay_partner(p):
        moved(p, partner, SIDE).wait_recv()
        if early(p):
            pl.when(z == 0)(lambda: moved(p, partner, RIGHT).start())
            pl.when(z == line - 1)(lambda: moved(p, partner, LEFT).start())

    def relay_corner(d, p):
        @pl.when(z == d)
        def _():
            moved(p, 1 - x, RIGHT).wait_recv()
            pl.when(has_right)(lambda: moved(p, 1 - x, RIGHT).start())

        @pl.when(z + d == line - 1)
        def _():
            origin = 2 * (line - 1) + 1 - x
            moved(p, origin, LEFT).wait_recv()
            pl.when(has_left)(lambda: moved(p, origin, LEFT).start())

    key_id = lax.broadcasted_iota(jnp.int32, (tok, 1), 0).astype(f32)
    dec_lane = lax.broadcasted_iota(jnp.int32, (1, dec_lanes), 1)
    small_copies[0].wait()
    dec_limit = jnp.zeros((1, dec_lanes), jnp.int32)
    for i in range(n_dec):
        dec_limit = jnp.where(
            jnp.logical_and(dec_lane % n_dec == i, dec_lane < GROUP * n_dec), pos_ref[i], dec_limit
        )
    dec_limit = dec_limit.astype(f32)
    query_row = (lax.broadcasted_iota(jnp.int32, (1, rows), 1) % tok).astype(f32)

    def weigh(block, h, diagonal=False):
        offset = own_off if diagonal else kbuf[block, 0, pl.ds(tok, MARK), :][0:1, 0:1].astype(f32)
        scores = lax.dot_general(
            kbuf[block, h, pl.ds(0, tok), :], qs[h], (((1,), (1,)), ((), ())),
            preferred_element_type=f32,
        )
        dec_seen = offset * tok + key_id < dec_limit
        dec_scores = jnp.where(dec_seen, scores[:, rows:], masked_score)
        scores = scores[:, :rows]
        if diagonal:
            scores = jnp.where(key_id <= query_row, scores, masked_score)
        old = m_ref[h][0:1]
        top = jnp.max(scores, axis=0, keepdims=True)
        new = jnp.maximum(old[:, :rows], top)
        if diagonal:
            used = new
        else:
            seen = offset <= own_off
            new = jnp.where(seen, new, old[:, :rows])
            used = jnp.where(seen, new, -masked_score)
        dec_new = jnp.maximum(old[:, rows:], jnp.max(dec_scores, axis=0, keepdims=True))
        new = jnp.concatenate([new, dec_new], axis=1)
        weights = jnp.concatenate([
            jnp.exp2((scores - used) * exp2_scale),
            jnp.exp2((dec_scores - dec_new) * exp2_scale),
        ], axis=1)
        factor = jnp.exp2((old - new) * exp2_scale)
        m_ref[h] = jnp.broadcast_to(new, m_ref.shape[1:])
        l_ref[h] = l_ref[h] * factor + jnp.sum(weights, axis=0, keepdims=True)
        return weights.astype(b16), factor

    def gather_values(block, h, weights, factor):
        added = lax.dot_general(
            vbuf[block, h], weights, (((0,), (0,)), ((), ())), preferred_element_type=f32
        )
        acc_ref[h] = acc_ref[h] * factor + added

    def attend(block, diagonal=False):
        weighed = [weigh(block, h, diagonal) for h in range(kv_heads)]
        for h in range(kv_heads):
            gather_values(block, h, *weighed[h])

    for copy in small_copies[1:]:
        copy.wait()
    pad = dec_lanes - GROUP * n_dec
    for h in range(kv_heads):
        q32 = jnp.concatenate([
            aq_ref[:, (h * GROUP + g) * HEAD_SIZE : (h * GROUP + g + 1) * HEAD_SIZE].astype(f32)
            for g in range(GROUP)
        ] + ([jnp.zeros((pad, HEAD_SIZE), f32)] if pad else []), axis=0)
        dec_q = q32.astype(b16)
        qs[h, pl.ds(rows, dec_lanes), :] = dec_q
        cols = slice(h * HEAD_SIZE, (h + 1) * HEAD_SIZE)
        own_lane = lax.broadcasted_iota(jnp.int32, (n_dec, dec_lanes), 1)
        own_token = lax.broadcasted_iota(jnp.int32, (n_dec, dec_lanes), 0)
        mine = jnp.logical_and(own_lane % n_dec == own_token, own_lane < GROUP * n_dec)
        pair_scores = lax.dot_general(
            ak_ref[:, cols], dec_q, (((1,), (1,)), ((), ())), preferred_element_type=f32
        )
        self_score = jnp.sum(jnp.where(mine, pair_scores, 0.0), axis=0, keepdims=True)
        picked = lax.dot_general(
            av_ref[:, cols].astype(f32), mine.astype(f32), (((0,), (0,)), ((), ())),
            preferred_element_type=f32,
        )
        m_ref[h] = jnp.broadcast_to(
            jnp.concatenate([jnp.full((1, rows), masked_score, f32), self_score], axis=1),
            m_ref.shape[1:],
        )
        l_ref[h] = jnp.concatenate(
            [jnp.zeros((8, rows), f32), jnp.ones((8, dec_lanes), f32)], axis=1
        )
        acc_ref[h] = jnp.concatenate([jnp.zeros((HEAD_SIZE, rows), f32), picked], axis=1)
    for copy in q_copies:
        copy.wait()
    attend(seq, diagonal=True)

    edge = jnp.logical_or(z == 0, z == line - 1)

    def near(d):
        pl.when(z >= d)(lambda: attend(2 * (z - d) + x))
        pl.when(z + d < line)(lambda: attend(2 * (z + d) + x))

    def await_side(d, h):
        for p in (2 * h, 2 * h + 1):
            if h == early_head:
                pl.when(z > d)(lambda: moved(p, 2 * (z - d) + 1 - x, SIDE).wait_recv())
                pl.when(z + d < line - 1)(
                    lambda: moved(p, 2 * (z + d) + 1 - x, SIDE).wait_recv()
                )
            else:
                pl.when(z >= d)(lambda: moved(p, 2 * (z - d) + 1 - x, SIDE).wait_recv())
                pl.when(z + d < line)(lambda: moved(p, 2 * (z + d) + 1 - x, SIDE).wait_recv())

    def across(d):
        for h in range(kv_heads):
            await_side(d, h)
        pl.when(z >= d)(lambda: attend(2 * (z - d) + 1 - x))
        pl.when(z + d < line)(lambda: attend(2 * (z + d) + 1 - x))

    corner_k, corner_v = 2 * early_head, 2 * early_head + 1

    for p in range(len(pieces)):
        relay_own(1, p)
        relay_partner(p)
    near(1)

    def round_(r, carry):
        for p in range(len(pieces)):
            relay_own(r, p)
            if p == 1:
                relay_corner(r - 1, corner_k)
                pl.when(both(r == 2, edge))(lambda: attend(partner))
                pl.when(both(r > 2, edge))(lambda: across(r - 2))
            if p == 2:
                relay_corner(r - 1, corner_v)
        near(r)
        pl.when(both(r == 2, jnp.logical_not(edge)))(lambda: attend(partner))
        pl.when(both(r > 2, jnp.logical_not(edge)))(lambda: across(r - 2))
        return carry

    lax.fori_loop(2, line, round_, 0)
    across(line - 2)

    def finish(origin):
        for h in range(kv_heads - 1):
            moved(2 * h, origin, SIDE).wait_recv()
        relay_corner(line - 1, corner_k)
        weighed = [weigh(origin, h) for h in range(kv_heads)]
        for h in range(kv_heads - 1):
            moved(2 * h + 1, origin, SIDE).wait_recv()
        relay_corner(line - 1, corner_v)
        for h in range(kv_heads):
            gather_values(origin, h, *weighed[h])

    pl.when(z == line - 1)(lambda: finish(1 - x))
    pl.when(z == 0)(lambda: finish(2 * (line - 1) + 1 - x))

    dec_pad = attn.shape[0] - tok - n_dec
    for h in range(kv_heads):
        turned = jnp.transpose(acc_ref[h] * (1.0 / l_ref[h][0:1]))
        for g in range(GROUP):
            i = h * GROUP + g
            cols = slice(i * HEAD_SIZE, (i + 1) * HEAD_SIZE)
            attn[0:tok, cols] = turned[g * tok : (g + 1) * tok].astype(b16)
            dec = turned[rows + g * n_dec : rows + (g + 1) * n_dec]
            if dec_pad:
                dec = jnp.concatenate([dec, jnp.zeros((dec_pad, HEAD_SIZE), f32)], axis=0)
            attn[tok:, cols] = dec.astype(b16)
    weight_copy.wait()

    n_chunk = model // chunk
    ahead = 2

    def core_copy(i):
        return pltpu.make_async_remote_copy(
            src_ref=send1.at[i], dst_ref=recv1.at[i], send_sem=ss1.at[i], recv_sem=rs1.at[i],
            device_id=to_core, device_id_type=MESH,
        )

    def y_copy(i):
        return pltpu.make_async_remote_copy(
            src_ref=send2.at[i], dst_ref=recv2.at[i], send_sem=ss2.at[i], recv_sem=rs2.at[i],
            device_id=to_y, device_id_type=MESH,
        )

    def block(index):
        return pl.ds(pl.multiple_of(index * part, 8), part)

    def pass_on(i):
        core_copy(i).wait_recv()
        total = own[i, 0:part] + recv1[i, 0:part].astype(f32)
        send2[i] = total.astype(b16)
        y_copy(i).start()

    def project(i, carry):
        cols = pl.ds(pl.multiple_of(i * chunk, chunk), chunk)
        pbuf[...] = jnp.dot(attn[...], wbuf[:, cols], preferred_element_type=f32)
        send1[i, 0:part] = pbuf[block(2 * (1 - y) + 1 - c)].astype(b16)
        send1[i, part:] = pbuf[block(2 * y + 1 - c)].astype(b16)
        core_copy(i).start()
        own[i, 0:part] = pbuf[block(2 * (1 - y) + c)]
        own[i, part:] = pbuf[block(2 * y + c)]
        dpart[:, cols] = pbuf[tok : tok + n_dec]
        pl.when(i >= ahead)(lambda: pass_on(i - ahead))
        return carry

    lax.fori_loop(0, n_chunk, project, 0)

    quarter = model // 4
    mine = pl.ds(seq * own_dec, own_dec)

    def dec_copy(way, peer):
        return pltpu.make_async_remote_copy(
            src_ref=dsend.at[way], dst_ref=drecv.at[way],
            send_sem=dss.at[way], recv_sem=drs.at[way],
            device_id=peer, device_id_type=MESH,
        )

    dec_copies = []
    for way, peer in enumerate((to_core, to_y, to_diag)):
        cols = pl.ds(pl.multiple_of(peer[1] * quarter, 128), quarter)
        dsend[way] = dpart[mine, cols]
        dec_copies.append(dec_copy(way, peer))
        dec_copies[-1].start()

    for i in range(n_chunk - ahead, n_chunk):
        pass_on(i)

    def drain(oz, carry):
        origin = 2 * oz + x
        edge = jnp.logical_or(oz == 0, oz == line - 1)
        for p in range(len(pieces)):
            pl.when(both(oz <= z, has_right))(lambda: moved(p, origin, RIGHT).wait_send())
            pl.when(both(oz >= z, has_left))(lambda: moved(p, origin, LEFT).wait_send())
            if early(p):
                pl.when(jnp.logical_or(oz == z, jnp.logical_not(edge)))(
                    lambda: moved(p, origin, SIDE).wait_send()
                )
            else:
                moved(p, origin, SIDE).wait_send()
        return carry

    lax.fori_loop(0, line, drain, 0)
    for p in (corner_k, corner_v):
        pl.when(has_right)(lambda: moved(p, 1 - x, RIGHT).wait_send())
        pl.when(has_left)(lambda: moved(p, 2 * (line - 1) + 1 - x, LEFT).wait_send())

    def gather_sum(i, carry):
        y_copy(i).wait_recv()
        cols = pl.ds(pl.multiple_of(i * chunk, chunk), chunk)
        total = own[i, part:] + recv1[i, part:].astype(f32)
        out_ref[:, cols] = (total + recv2[i].astype(f32)).astype(b16)
        y_copy(i).wait_send()
        core_copy(i).wait_send()
        return carry

    lax.fori_loop(0, n_chunk, gather_sum, 0)
    for copy in dec_copies:
        copy.wait()
    dec_total = dpart[mine, pl.ds(pl.multiple_of(head * quarter, 128), quarter)]
    dec_total = dec_total + drecv[0] + drecv[1] + drecv[2]
    dec_ref[...] = jnp.broadcast_to(dec_total, dec_ref.shape)


def on_device(
    prompt_queries, prompt_keys, prompt_values, span_offset,
    appended_queries, appended_keys, appended_values, dec_pos, out_weight,
):
    n_seq = lax.axis_size("seq")
    tok, width = prompt_queries.shape
    kv_width = prompt_keys.shape[1]
    kv_heads = kv_width // HEAD_SIZE
    heads = kv_heads * GROUP
    n_dec = appended_queries.shape[0]
    own_dec = n_dec // n_seq
    model = out_weight.shape[1]
    chunk = 512
    n_chunk = model // chunk
    part = tok // 4
    rows = tok + -(-n_dec // 16) * 16
    lanes = GROUP * tok + -(-GROUP * n_dec // LANES) * LANES
    vmem = pl.BlockSpec(memory_space=pltpu.VMEM)
    hbm = pl.BlockSpec(memory_space=pltpu.MemorySpace.HBM)
    smem = pl.BlockSpec(memory_space=pltpu.SMEM)
    f32, b16 = jnp.float32, jnp.bfloat16
    dma = pltpu.SemaphoreType.DMA
    n_piece = 2 * kv_heads
    results = pl.pallas_call(
        functools.partial(kernel, n_seq, own_dec, chunk, n_dec, tok),
        out_shape=(
            jax.ShapeDtypeStruct((part, model), b16),
            jax.ShapeDtypeStruct((8 * own_dec, model // 4), f32),
        ),
        in_specs=[hbm] * 3 + [smem] + [hbm] * 5,
        out_specs=(vmem, vmem),
        scratch_shapes=[
            pltpu.VMEM((n_seq, kv_heads, tok + MARK, HEAD_SIZE), b16),
            pltpu.VMEM((n_seq, kv_heads, tok, HEAD_SIZE), b16),
            pltpu.VMEM(out_weight.shape, b16),
            pltpu.VMEM((kv_heads, lanes, HEAD_SIZE), b16),
            pltpu.VMEM((n_dec, width), b16),
            pltpu.VMEM((n_dec, kv_width), b16),
            pltpu.VMEM((n_dec, kv_width), b16),
            pltpu.VMEM((kv_heads, 8, lanes), f32),
            pltpu.VMEM((kv_heads, 8, lanes), f32),
            pltpu.VMEM((kv_heads, HEAD_SIZE, lanes), f32),
            pltpu.SMEM((n_dec,), jnp.int32),
            pltpu.VMEM((rows, width), b16),
            pltpu.VMEM((rows, chunk), f32),
            pltpu.VMEM((n_chunk, 2 * part, chunk), f32),
            pltpu.VMEM((n_chunk, 2 * part, chunk), b16),
            pltpu.VMEM((n_chunk, 2 * part, chunk), b16),
            pltpu.VMEM((n_chunk, part, chunk), b16),
            pltpu.VMEM((n_chunk, part, chunk), b16),
            pltpu.VMEM((n_dec, model), f32),
            pltpu.VMEM((3, own_dec, model // 4), f32),
            pltpu.VMEM((3, own_dec, model // 4), f32),
            dma((n_piece,)), dma((heads,)), dma((4,)), dma,
            dma((3, n_piece, n_seq)), dma((n_piece, n_seq)),
            dma((n_chunk,)), dma((n_chunk,)), dma((n_chunk,)), dma((n_chunk,)),
            dma((3,)), dma((3,)),
        ],
        compiler_params=pltpu.CompilerParams(
            collective_id=0, has_side_effects=True, vmem_limit_bytes=44 * 2**20
        ),
    )(
        *map(in_hbm, (prompt_queries, prompt_keys, prompt_values)), span_offset,
        *map(in_hbm, (appended_queries, appended_keys, appended_values, dec_pos, out_weight)),
    )
    return pl.pallas_call(
        hand_on,
        out_shape=(
            jax.ShapeDtypeStruct((part, model), b16),
            jax.ShapeDtypeStruct((own_dec, model // 4), b16),
        ),
        in_specs=[vmem] * 2,
        out_specs=(vmem, vmem),
        compiler_params=pltpu.CompilerParams(vmem_limit_bytes=4 * 2**20),
    )(*results)


def solution(mesh):
    in_specs = (
        P("seq", "head"),
        P("seq", "head"),
        P("seq", "head"),
        P("seq"),
        P(None, "head"),
        P(None, "head"),
        P(None, "head"),
        P(),
        P("head", None),
    )
    out_specs = (P(("seq", "head"), None), P("seq", "head"))
    return jax.shard_map(
        on_device, mesh=mesh, in_specs=in_specs, out_specs=out_specs, check_vma=False
    )
```

```python
import functools
import math

import jax
import jax.numpy as jnp
from jax import lax
from jax.experimental import pallas as pl
from jax.experimental.pallas import tpu as pltpu
from jax.sharding import PartitionSpec as P

QUERY_HEADS = 32
KEY_VALUE_HEADS = 8
HEAD_SIZE = 128
GROUP = QUERY_HEADS // KEY_VALUE_HEADS
MESH = pl.DeviceIdType.MESH
LANES = 128
MARK = 16

masked_score = -1e30
exp2_scale = HEAD_SIZE ** (-0.5) * math.log2(math.e)
LEFT, RIGHT, SIDE = 0, 1, 2


def hand_on(layer_in, dec_in, layer_out, dec_out):
    layer_out[...] = layer_in[...]
    dec_out[...] = dec_in[0 : dec_out.shape[0]].astype(dec_out.dtype)


def in_hbm(array):
    return pltpu.with_memory_space_constraint(array, pltpu.MemorySpace.HBM)


def both(*conditions):
    result = conditions[0]
    for condition in conditions[1:]:
        result = jnp.logical_and(result, condition)
    return result


def kernel(
    n_seq, own_dec, chunk, n_dec, tok,
    q_hbm, k_hbm, v_hbm, span_ref, aq_hbm, ak_hbm, av_hbm, pos_hbm, w_hbm,
    out_ref, dec_ref,
    kbuf, vbuf, wbuf, qs, aq_ref, ak_ref, av_ref, m_ref, l_ref, acc_ref,
    pos_ref, attn, pbuf, own, send1, recv1, send2, recv2,
    xown, xsend, xrecv, dpart, dsend, drecv,
    kv_sem, q_sem, a_sem, w_sem, ss, rs, ss1, rs1, ss2, rs2, dss, drs, xss, xrs,
):
    kv_heads = kbuf.shape[1]
    model = w_hbm.shape[1]
    part = tok // 4
    line = n_seq // 2
    rows = GROUP * tok
    lanes = qs.shape[1]
    dec_lanes = lanes - rows
    f32, b16 = jnp.float32, jnp.bfloat16
    seq = lax.axis_index("seq")
    head = lax.axis_index("head")
    z, x = seq // 2, seq % 2
    y, c = head // 2, head % 2
    partner = 2 * z + 1 - x
    to_x = (partner, head)
    to_right = (jnp.minimum(seq + 2, n_seq - 1), head)
    to_left = (jnp.maximum(seq - 2, 0), head)
    to_core = (seq, 2 * y + 1 - c)
    to_y = (seq, 2 * (1 - y) + c)
    to_diag = (seq, 2 * (1 - y) + 1 - c)
    has_left, has_right = z > 0, z < line - 1
    targets = (to_left, to_right, to_x)

    barrier = pltpu.get_barrier_semaphore()
    for peer in (to_x, to_core, to_y, to_diag):
        pl.semaphore_signal(barrier, inc=1, device_id=peer, device_id_type=MESH)
    pl.when(has_left)(
        lambda: pl.semaphore_signal(barrier, inc=1, device_id=to_left, device_id_type=MESH)
    )
    pl.when(has_right)(
        lambda: pl.semaphore_signal(barrier, inc=1, device_id=to_right, device_id_type=MESH)
    )

    pieces = [(h, kind) for h in range(kv_heads) for kind in (0, 1)]
    early_head = kv_heads - 1

    def column(ref, i):
        return ref.at[:, pl.ds(i * HEAD_SIZE, HEAD_SIZE)]

    kv_copies = []
    for p, (h, kind) in enumerate(pieces):
        source, buffer = ((k_hbm, kbuf), (v_hbm, vbuf))[kind]
        kv_copies.append(pltpu.make_async_copy(
            column(source, h), buffer.at[seq, h, pl.ds(0, tok)], kv_sem.at[p]
        ))
        kv_copies[-1].start()
    small_copies = [
        pltpu.make_async_copy(source, buffer, a_sem.at[i])
        for i, (source, buffer) in enumerate(
            (
                (pos_hbm, pos_ref), (aq_hbm, aq_ref),
                (ak_hbm, ak_ref), (av_hbm, av_ref),
            )
        )
    ]
    for copy in small_copies:
        copy.start()
    q_copies = []
    for h in range(kv_heads):
        for g in range(GROUP):
            i = h * GROUP + g
            q_copies.append(pltpu.make_async_copy(
                column(q_hbm, i), qs.at[h, pl.ds(g * tok, tok)], q_sem.at[i]
            ))
            q_copies[-1].start()
    weight_copy = pltpu.make_async_copy(w_hbm, wbuf, w_sem)
    weight_copy.start()

    own_mark = jnp.full((MARK, LANES), span_ref[0], jnp.int32).astype(f32)
    kbuf[seq, 0, pl.ds(tok, MARK), :] = own_mark.astype(b16)
    own_off = own_mark[0:1, 0:1]
    pl.semaphore_wait(barrier, 4 + jnp.where(has_left, 1, 0) + jnp.where(has_right, 1, 0))

    def moved(p, origin, way):
        h, kind = pieces[p]
        count = tok + MARK if p == 0 else tok
        slot = (kbuf, vbuf)[kind].at[origin, h, pl.ds(0, count)]
        return pltpu.make_async_remote_copy(
            src_ref=slot, dst_ref=slot,
            send_sem=ss.at[way, p, origin], recv_sem=rs.at[p, origin],
            device_id=targets[way], device_id_type=MESH,
        )

    def early(p):
        return pieces[p][0] == early_head

    for copy in kv_copies:
        copy.wait()
    sideways = [(p + 2) % len(pieces) for p in range(len(pieces))]
    for p in range(len(pieces)):
        moved(sideways[p], seq, SIDE).start()
        pl.when(has_left)(lambda: moved(p, seq, LEFT).start())
        pl.when(has_right)(lambda: moved(p, seq, RIGHT).start())

    def relay_own(d, p):
        @pl.when(z >= d)
        def _():
            origin = 2 * (z - d) + x
            moved(p, origin, RIGHT).wait_recv()
            pl.when(has_right)(lambda: moved(p, origin, RIGHT).start())
            if early(p):
                pl.when(z != d)(lambda: moved(p, origin, SIDE).start())
            else:
                moved(p, origin, SIDE).start()

        @pl.when(z + d < line)
        def _():
            origin = 2 * (z + d) + x
            moved(p, origin, LEFT).wait_recv()
            pl.when(has_left)(lambda: moved(p, origin, LEFT).start())
            if early(p):
                pl.when(z + d != line - 1)(lambda: moved(p, origin, SIDE).start())
            else:
                moved(p, origin, SIDE).start()

    def relay_partner(p):
        moved(p, partner, SIDE).wait_recv()
        if early(p):
            pl.when(z == 0)(lambda: moved(p, partner, RIGHT).start())
            pl.when(z == line - 1)(lambda: moved(p, partner, LEFT).start())

    def relay_corner(d, p):
        @pl.when(z == d)
        def _():
            moved(p, 1 - x, RIGHT).wait_recv()
            pl.when(has_right)(lambda: moved(p, 1 - x, RIGHT).start())

        @pl.when(z + d == line - 1)
        def _():
            origin = 2 * (line - 1) + 1 - x
            moved(p, origin, LEFT).wait_recv()
            pl.when(has_left)(lambda: moved(p, origin, LEFT).start())

    key_id = lax.broadcasted_iota(jnp.int32, (tok, 1), 0).astype(f32)
    dec_lane = lax.broadcasted_iota(jnp.int32, (1, dec_lanes), 1)
    small_copies[0].wait()
    dec_limit = jnp.zeros((1, dec_lanes), jnp.int32)
    for i in range(n_dec):
        dec_limit = jnp.where(
            jnp.logical_and(dec_lane % n_dec == i, dec_lane < GROUP * n_dec), pos_ref[i], dec_limit
        )
    dec_limit = dec_limit.astype(f32)
    query_row = (lax.broadcasted_iota(jnp.int32, (1, rows), 1) % tok).astype(f32)

    def weigh(block, h, diagonal=False):
        offset = own_off if diagonal else kbuf[block, 0, pl.ds(tok, MARK), :][0:1, 0:1].astype(f32)
        scores = lax.dot_general(
            kbuf[block, h, pl.ds(0, tok), :], qs[h], (((1,), (1,)), ((), ())),
            preferred_element_type=f32,
        )
        dec_seen = offset * tok + key_id < dec_limit
        dec_scores = jnp.where(dec_seen, scores[:, rows:], masked_score)
        scores = scores[:, :rows]
        if diagonal:
            scores = jnp.where(key_id <= query_row, scores, masked_score)
        old = m_ref[h][0:1]
        top = jnp.max(scores, axis=0, keepdims=True)
        new = jnp.maximum(old[:, :rows], top)
        if diagonal:
            used = new
        else:
            seen = offset <= own_off
            new = jnp.where(seen, new, old[:, :rows])
            used = jnp.where(seen, new, -masked_score)
        dec_new = jnp.maximum(old[:, rows:], jnp.max(dec_scores, axis=0, keepdims=True))
        new = jnp.concatenate([new, dec_new], axis=1)
        weights = jnp.concatenate([
            jnp.exp2((scores - used) * exp2_scale),
            jnp.exp2((dec_scores - dec_new) * exp2_scale),
        ], axis=1)
        factor = jnp.exp2((old - new) * exp2_scale)
        m_ref[h] = jnp.broadcast_to(new, m_ref.shape[1:])
        l_ref[h] = l_ref[h] * factor + jnp.sum(weights, axis=0, keepdims=True)
        return weights.astype(b16), factor

    def gather_values(block, h, weights, factor):
        added = lax.dot_general(
            vbuf[block, h], weights, (((0,), (0,)), ((), ())), preferred_element_type=f32
        )
        acc_ref[h] = acc_ref[h] * factor + added

    def attend(block, diagonal=False):
        weighed = [weigh(block, h, diagonal) for h in range(kv_heads)]
        for h in range(kv_heads):
            gather_values(block, h, *weighed[h])

    for copy in small_copies[1:]:
        copy.wait()
    pad = dec_lanes - GROUP * n_dec
    for h in range(kv_heads):
        q32 = jnp.concatenate([
            aq_ref[:, (h * GROUP + g) * HEAD_SIZE : (h * GROUP + g + 1) * HEAD_SIZE].astype(f32)
            for g in range(GROUP)
        ] + ([jnp.zeros((pad, HEAD_SIZE), f32)] if pad else []), axis=0)
        dec_q = q32.astype(b16)
        qs[h, pl.ds(rows, dec_lanes), :] = dec_q
        cols = slice(h * HEAD_SIZE, (h + 1) * HEAD_SIZE)
        own_lane = lax.broadcasted_iota(jnp.int32, (n_dec, dec_lanes), 1)
        own_token = lax.broadcasted_iota(jnp.int32, (n_dec, dec_lanes), 0)
        mine = jnp.logical_and(own_lane % n_dec == own_token, own_lane < GROUP * n_dec)
        pair_scores = lax.dot_general(
            ak_ref[:, cols], dec_q, (((1,), (1,)), ((), ())), preferred_element_type=f32
        )
        self_score = jnp.sum(jnp.where(mine, pair_scores, 0.0), axis=0, keepdims=True)
        picked = lax.dot_general(
            av_ref[:, cols].astype(f32), mine.astype(f32), (((0,), (0,)), ((), ())),
            preferred_element_type=f32,
        )
        m_ref[h] = jnp.broadcast_to(
            jnp.concatenate([jnp.full((1, rows), masked_score, f32), self_score], axis=1),
            m_ref.shape[1:],
        )
        l_ref[h] = jnp.concatenate(
            [jnp.zeros((8, rows), f32), jnp.ones((8, dec_lanes), f32)], axis=1
        )
        acc_ref[h] = jnp.concatenate([jnp.zeros((HEAD_SIZE, rows), f32), picked], axis=1)
    for copy in q_copies:
        copy.wait()
    attend(seq, diagonal=True)

    edge = jnp.logical_or(z == 0, z == line - 1)

    def near(d):
        pl.when(z >= d)(lambda: attend(2 * (z - d) + x))
        pl.when(z + d < line)(lambda: attend(2 * (z + d) + x))

    def await_side(d, h):
        for p in (2 * h, 2 * h + 1):
            if h == early_head:
                pl.when(z > d)(lambda: moved(p, 2 * (z - d) + 1 - x, SIDE).wait_recv())
                pl.when(z + d < line - 1)(
                    lambda: moved(p, 2 * (z + d) + 1 - x, SIDE).wait_recv()
                )
            else:
                pl.when(z >= d)(lambda: moved(p, 2 * (z - d) + 1 - x, SIDE).wait_recv())
                pl.when(z + d < line)(lambda: moved(p, 2 * (z + d) + 1 - x, SIDE).wait_recv())

    def across(d):
        for h in range(kv_heads):
            await_side(d, h)
        pl.when(z >= d)(lambda: attend(2 * (z - d) + 1 - x))
        pl.when(z + d < line)(lambda: attend(2 * (z + d) + 1 - x))

    corner_k, corner_v = 2 * early_head, 2 * early_head + 1

    for p in range(len(pieces)):
        relay_own(1, p)
        relay_partner(sideways[p])
    near(1)

    def round_(r, carry):
        for p in range(len(pieces)):
            relay_own(r, p)
            if p == 1:
                relay_corner(r - 1, corner_k)
                pl.when(both(r == 2, edge))(lambda: attend(partner))
                pl.when(both(r > 2, edge))(lambda: across(r - 2))
            if p == 2:
                relay_corner(r - 1, corner_v)
        near(r)
        pl.when(both(r == 2, jnp.logical_not(edge)))(lambda: attend(partner))
        pl.when(both(r > 2, jnp.logical_not(edge)))(lambda: across(r - 2))
        return carry

    lax.fori_loop(2, line, round_, 0)
    across(line - 2)

    def finish(origin):
        for h in range(kv_heads - 1):
            moved(2 * h, origin, SIDE).wait_recv()
        relay_corner(line - 1, corner_k)
        weighed = [weigh(origin, h) for h in range(kv_heads)]
        for h in range(kv_heads - 1):
            moved(2 * h + 1, origin, SIDE).wait_recv()
        relay_corner(line - 1, corner_v)
        for h in range(kv_heads):
            gather_values(origin, h, *weighed[h])

    pl.when(z == line - 1)(lambda: finish(1 - x))
    pl.when(z == 0)(lambda: finish(2 * (line - 1) + 1 - x))

    dec_pad = attn.shape[0] - tok - n_dec
    for h in range(kv_heads):
        turned = jnp.transpose(acc_ref[h] * (1.0 / l_ref[h][0:1]))
        for g in range(GROUP):
            i = h * GROUP + g
            cols = slice(i * HEAD_SIZE, (i + 1) * HEAD_SIZE)
            attn[0:tok, cols] = turned[g * tok : (g + 1) * tok].astype(b16)
            dec = turned[rows + g * n_dec : rows + (g + 1) * n_dec]
            if dec_pad:
                dec = jnp.concatenate([dec, jnp.zeros((dec_pad, HEAD_SIZE), f32)], axis=0)
            attn[tok:, cols] = dec.astype(b16)
    weight_copy.wait()

    direct = xown.shape[1]
    n_chunk = (model - direct) // chunk
    ahead = 2

    def core_copy(i):
        return pltpu.make_async_remote_copy(
            src_ref=send1.at[i], dst_ref=recv1.at[i], send_sem=ss1.at[i], recv_sem=rs1.at[i],
            device_id=to_core, device_id_type=MESH,
        )

    def y_copy(i):
        return pltpu.make_async_remote_copy(
            src_ref=send2.at[i], dst_ref=recv2.at[i], send_sem=ss2.at[i], recv_sem=rs2.at[i],
            device_id=to_y, device_id_type=MESH,
        )

    def block(index):
        return pl.ds(pl.multiple_of(index * part, 8), part)

    def columns(i):
        return pl.ds(pl.multiple_of(direct + i * chunk, LANES), chunk)

    first = slice(0, direct)
    pbuf[:, first] = jnp.dot(attn[...], wbuf[:, first], preferred_element_type=f32)
    first_copies = []
    for way, (peer, owner) in enumerate((
        (to_y, 2 * (1 - y) + c), (to_diag, 2 * (1 - y) + 1 - c), (to_core, 2 * y + 1 - c),
    )):
        xsend[way] = pbuf[block(owner), first].astype(b16)
        first_copies.append(pltpu.make_async_remote_copy(
            src_ref=xsend.at[way], dst_ref=xrecv.at[way],
            send_sem=xss.at[way], recv_sem=xrs.at[way],
            device_id=peer, device_id_type=MESH,
        ))
        first_copies[-1].start()
    xown[...] = pbuf[block(2 * y + c), first]
    dpart[:, first] = pbuf[tok : tok + n_dec, first]

    def pass_on(i):
        core_copy(i).wait_recv()
        total = own[i, 0:part] + recv1[i, 0:part].astype(f32)
        send2[i] = total.astype(b16)
        y_copy(i).start()

    def project(i, carry):
        cols = columns(i)
        pbuf[:, 0:chunk] = jnp.dot(attn[...], wbuf[:, cols], preferred_element_type=f32)
        send1[i, 0:part] = pbuf[block(2 * (1 - y) + 1 - c), 0:chunk].astype(b16)
        send1[i, part:] = pbuf[block(2 * y + 1 - c), 0:chunk].astype(b16)
        core_copy(i).start()
        own[i, 0:part] = pbuf[block(2 * (1 - y) + c), 0:chunk]
        own[i, part:] = pbuf[block(2 * y + c), 0:chunk]
        dpart[:, cols] = pbuf[tok : tok + n_dec, 0:chunk]
        pl.when(i >= ahead)(lambda: pass_on(i - ahead))
        return carry

    lax.fori_loop(0, n_chunk, project, 0)

    quarter = model // 4
    mine = pl.ds(seq * own_dec, own_dec)

    def dec_copy(way, peer):
        return pltpu.make_async_remote_copy(
            src_ref=dsend.at[way], dst_ref=drecv.at[way],
            send_sem=dss.at[way], recv_sem=drs.at[way],
            device_id=peer, device_id_type=MESH,
        )

    dec_copies = []
    for way, peer in enumerate((to_core, to_y, to_diag)):
        cols = pl.ds(pl.multiple_of(peer[1] * quarter, 128), quarter)
        dsend[way] = dpart[mine, cols]
        dec_copies.append(dec_copy(way, peer))
        dec_copies[-1].start()

    for i in range(n_chunk - ahead, n_chunk):
        pass_on(i)

    def drain(oz, carry):
        origin = 2 * oz + x
        edge = jnp.logical_or(oz == 0, oz == line - 1)
        for p in range(len(pieces)):
            pl.when(both(oz <= z, has_right))(lambda: moved(p, origin, RIGHT).wait_send())
            pl.when(both(oz >= z, has_left))(lambda: moved(p, origin, LEFT).wait_send())
            if early(p):
                pl.when(jnp.logical_or(oz == z, jnp.logical_not(edge)))(
                    lambda: moved(p, origin, SIDE).wait_send()
                )
            else:
                moved(p, origin, SIDE).wait_send()
        return carry

    lax.fori_loop(0, line, drain, 0)
    for p in (corner_k, corner_v):
        pl.when(has_right)(lambda: moved(p, 1 - x, RIGHT).wait_send())
        pl.when(has_left)(lambda: moved(p, 2 * (line - 1) + 1 - x, LEFT).wait_send())

    def gather_sum(i, carry):
        y_copy(i).wait_recv()
        cols = columns(i)
        total = own[i, part:] + recv1[i, part:].astype(f32)
        out_ref[:, cols] = (total + recv2[i].astype(f32)).astype(b16)
        y_copy(i).wait_send()
        core_copy(i).wait_send()
        return carry

    for copy in first_copies:
        copy.wait()
    total = xown[...]
    for way in range(3):
        total = total + xrecv[way].astype(f32)
    out_ref[:, first] = total.astype(b16)
    lax.fori_loop(0, n_chunk, gather_sum, 0)
    for copy in dec_copies:
        copy.wait()
    dec_total = dpart[mine, pl.ds(pl.multiple_of(head * quarter, 128), quarter)]
    dec_total = dec_total + drecv[0] + drecv[1] + drecv[2]
    dec_ref[...] = jnp.broadcast_to(dec_total, dec_ref.shape)


def on_device(
    prompt_queries, prompt_keys, prompt_values, span_offset,
    appended_queries, appended_keys, appended_values, dec_pos, out_weight,
):
    n_seq = lax.axis_size("seq")
    tok, width = prompt_queries.shape
    kv_width = prompt_keys.shape[1]
    kv_heads = kv_width // HEAD_SIZE
    heads = kv_heads * GROUP
    n_dec = appended_queries.shape[0]
    own_dec = n_dec // n_seq
    model = out_weight.shape[1]
    direct = 4 * LANES
    chunk = next(c for c in (512, 384, 256, LANES) if (model - direct) % c == 0)
    n_chunk = (model - direct) // chunk
    part = tok // 4
    rows = tok + -(-n_dec // 16) * 16
    lanes = GROUP * tok + -(-GROUP * n_dec // LANES) * LANES
    vmem = pl.BlockSpec(memory_space=pltpu.VMEM)
    hbm = pl.BlockSpec(memory_space=pltpu.MemorySpace.HBM)
    smem = pl.BlockSpec(memory_space=pltpu.SMEM)
    f32, b16 = jnp.float32, jnp.bfloat16
    dma = pltpu.SemaphoreType.DMA
    n_piece = 2 * kv_heads
    results = pl.pallas_call(
        functools.partial(kernel, n_seq, own_dec, chunk, n_dec, tok),
        out_shape=(
            jax.ShapeDtypeStruct((part, model), b16),
            jax.ShapeDtypeStruct((8 * own_dec, model // 4), f32),
        ),
        in_specs=[hbm] * 3 + [smem] + [hbm] * 5,
        out_specs=(vmem, vmem),
        scratch_shapes=[
            pltpu.VMEM((n_seq, kv_heads, tok + MARK, HEAD_SIZE), b16),
            pltpu.VMEM((n_seq, kv_heads, tok, HEAD_SIZE), b16),
            pltpu.VMEM(out_weight.shape, b16),
            pltpu.VMEM((kv_heads, lanes, HEAD_SIZE), b16),
            pltpu.VMEM((n_dec, width), b16),
            pltpu.VMEM((n_dec, kv_width), b16),
            pltpu.VMEM((n_dec, kv_width), b16),
            pltpu.VMEM((kv_heads, 8, lanes), f32),
            pltpu.VMEM((kv_heads, 8, lanes), f32),
            pltpu.VMEM((kv_heads, HEAD_SIZE, lanes), f32),
            pltpu.SMEM((n_dec,), jnp.int32),
            pltpu.VMEM((rows, width), b16),
            pltpu.VMEM((rows, max(chunk, direct)), f32),
            pltpu.VMEM((n_chunk, 2 * part, chunk), f32),
            pltpu.VMEM((n_chunk, 2 * part, chunk), b16),
            pltpu.VMEM((n_chunk, 2 * part, chunk), b16),
            pltpu.VMEM((n_chunk, part, chunk), b16),
            pltpu.VMEM((n_chunk, part, chunk), b16),
            pltpu.VMEM((part, direct), f32),
            pltpu.VMEM((3, part, direct), b16),
            pltpu.VMEM((3, part, direct), b16),
            pltpu.VMEM((n_dec, model), f32),
            pltpu.VMEM((3, own_dec, model // 4), f32),
            pltpu.VMEM((3, own_dec, model // 4), f32),
            dma((n_piece,)), dma((heads,)), dma((4,)), dma,
            dma((3, n_piece, n_seq)), dma((n_piece, n_seq)),
            dma((n_chunk,)), dma((n_chunk,)), dma((n_chunk,)), dma((n_chunk,)),
            dma((3,)), dma((3,)), dma((3,)), dma((3,)),
        ],
        compiler_params=pltpu.CompilerParams(
            collective_id=0, has_side_effects=True, vmem_limit_bytes=44 * 2**20
        ),
    )(
        *map(in_hbm, (prompt_queries, prompt_keys, prompt_values)), span_offset,
        *map(in_hbm, (appended_queries, appended_keys, appended_values, dec_pos, out_weight)),
    )
    return pl.pallas_call(
        hand_on,
        out_shape=(
            jax.ShapeDtypeStruct((part, model), b16),
            jax.ShapeDtypeStruct((own_dec, model // 4), b16),
        ),
        in_specs=[vmem] * 2,
        out_specs=(vmem, vmem),
        compiler_params=pltpu.CompilerParams(vmem_limit_bytes=4 * 2**20),
    )(*results)


def solution(mesh):
    in_specs = (
        P("seq", "head"),
        P("seq", "head"),
        P("seq", "head"),
        P("seq"),
        P(None, "head"),
        P(None, "head"),
        P(None, "head"),
        P(),
        P("head", None),
    )
    out_specs = (P(("seq", "head"), None), P("seq", "head"))
    return jax.shard_map(
        on_device, mesh=mesh, in_specs=in_specs, out_specs=out_specs, check_vma=False
    )
```

```python
import functools
import math

import jax
import jax.numpy as jnp
from jax import lax
from jax.experimental import pallas as pl
from jax.experimental.pallas import tpu as pltpu
from jax.sharding import PartitionSpec as P

QUERY_HEADS = 32
KEY_VALUE_HEADS = 8
HEAD_SIZE = 128
GROUP = QUERY_HEADS // KEY_VALUE_HEADS
MESH = pl.DeviceIdType.MESH
LANES = 128
MARK = 16

masked_score = -1e30
exp2_scale = HEAD_SIZE ** (-0.5) * math.log2(math.e)
LEFT, RIGHT, SIDE = 0, 1, 2


def hand_on(layer_in, dec_in, layer_out, dec_out):
    layer_out[...] = layer_in[...]
    dec_out[...] = dec_in[0 : dec_out.shape[0]].astype(dec_out.dtype)


def in_hbm(array):
    return pltpu.with_memory_space_constraint(array, pltpu.MemorySpace.HBM)


def both(*conditions):
    result = conditions[0]
    for condition in conditions[1:]:
        result = jnp.logical_and(result, condition)
    return result


def kernel(
    n_seq, own_dec, chunk, n_dec, tok,
    q_hbm, k_hbm, v_hbm, span_ref, aq_hbm, ak_hbm, av_hbm, pos_hbm, w_hbm,
    out_ref, dec_ref,
    kbuf, vbuf, wbuf, qs, aq_ref, ak_ref, av_ref, m_ref, l_ref, acc_ref,
    pos_ref, attn, pbuf, own, send1, recv1, send2, recv2,
    xown, xsend, xrecv, dpart, dsend, drecv,
    kv_sem, q_sem, a_sem, w_sem, ss, rs, ss1, rs1, ss2, rs2, dss, drs, xss, xrs,
):
    kv_heads = kbuf.shape[1]
    model = w_hbm.shape[1]
    part = tok // 4
    line = n_seq // 2
    rows = GROUP * tok
    lanes = qs.shape[1]
    dec_lanes = lanes - rows
    f32, b16 = jnp.float32, jnp.bfloat16
    seq = lax.axis_index("seq")
    head = lax.axis_index("head")
    z, x = seq // 2, seq % 2
    y, c = head // 2, head % 2
    partner = 2 * z + 1 - x
    to_x = (partner, head)
    to_right = (jnp.minimum(seq + 2, n_seq - 1), head)
    to_left = (jnp.maximum(seq - 2, 0), head)
    to_core = (seq, 2 * y + 1 - c)
    to_y = (seq, 2 * (1 - y) + c)
    to_diag = (seq, 2 * (1 - y) + 1 - c)
    has_left, has_right = z > 0, z < line - 1
    targets = (to_left, to_right, to_x)

    barrier = pltpu.get_barrier_semaphore()
    for peer in (to_x, to_core, to_y, to_diag):
        pl.semaphore_signal(barrier, inc=1, device_id=peer, device_id_type=MESH)
    pl.when(has_left)(
        lambda: pl.semaphore_signal(barrier, inc=1, device_id=to_left, device_id_type=MESH)
    )
    pl.when(has_right)(
        lambda: pl.semaphore_signal(barrier, inc=1, device_id=to_right, device_id_type=MESH)
    )

    pieces = [(h, kind) for h in range(kv_heads) for kind in (0, 1)]
    early_head = kv_heads - 1

    def column(ref, i):
        return ref.at[:, pl.ds(i * HEAD_SIZE, HEAD_SIZE)]

    kv_copies = []
    for p, (h, kind) in enumerate(pieces):
        source, buffer = ((k_hbm, kbuf), (v_hbm, vbuf))[kind]
        kv_copies.append(pltpu.make_async_copy(
            column(source, h), buffer.at[seq, h, pl.ds(0, tok)], kv_sem.at[p]
        ))
        kv_copies[-1].start()
    small_copies = [
        pltpu.make_async_copy(source, buffer, a_sem.at[i])
        for i, (source, buffer) in enumerate(
            (
                (pos_hbm, pos_ref), (aq_hbm, aq_ref),
                (ak_hbm, ak_ref), (av_hbm, av_ref),
            )
        )
    ]
    for copy in small_copies:
        copy.start()
    q_copies = []
    for h in range(kv_heads):
        for g in range(GROUP):
            i = h * GROUP + g
            q_copies.append(pltpu.make_async_copy(
                column(q_hbm, i), qs.at[h, pl.ds(g * tok, tok)], q_sem.at[i]
            ))
            q_copies[-1].start()
    weight_copy = pltpu.make_async_copy(w_hbm, wbuf, w_sem)
    weight_copy.start()

    own_mark = jnp.full((MARK, LANES), span_ref[0], jnp.int32).astype(f32)
    kbuf[seq, 0, pl.ds(tok, MARK), :] = own_mark.astype(b16)
    own_off = own_mark[0:1, 0:1]
    pl.semaphore_wait(barrier, 4 + jnp.where(has_left, 1, 0) + jnp.where(has_right, 1, 0))

    def moved(p, origin, way):
        h, kind = pieces[p]
        count = tok + MARK if p == 0 else tok
        slot = (kbuf, vbuf)[kind].at[origin, h, pl.ds(0, count)]
        return pltpu.make_async_remote_copy(
            src_ref=slot, dst_ref=slot,
            send_sem=ss.at[way, p, origin], recv_sem=rs.at[p, origin],
            device_id=targets[way], device_id_type=MESH,
        )

    def early(p):
        return pieces[p][0] == early_head

    for copy in kv_copies:
        copy.wait()
    sideways = [(p + 2) % len(pieces) for p in range(len(pieces))]
    for p in range(len(pieces)):
        moved(sideways[p], seq, SIDE).start()
        pl.when(has_left)(lambda: moved(p, seq, LEFT).start())
        pl.when(has_right)(lambda: moved(p, seq, RIGHT).start())

    def relay_own(d, p):
        @pl.when(z >= d)
        def _():
            origin = 2 * (z - d) + x
            moved(p, origin, RIGHT).wait_recv()
            pl.when(has_right)(lambda: moved(p, origin, RIGHT).start())
            if early(p):
                pl.when(z != d)(lambda: moved(p, origin, SIDE).start())
            else:
                moved(p, origin, SIDE).start()

        @pl.when(z + d < line)
        def _():
            origin = 2 * (z + d) + x
            moved(p, origin, LEFT).wait_recv()
            pl.when(has_left)(lambda: moved(p, origin, LEFT).start())
            if early(p):
                pl.when(z + d != line - 1)(lambda: moved(p, origin, SIDE).start())
            else:
                moved(p, origin, SIDE).start()

    def relay_partner(p):
        moved(p, partner, SIDE).wait_recv()
        if early(p):
            pl.when(z == 0)(lambda: moved(p, partner, RIGHT).start())
            pl.when(z == line - 1)(lambda: moved(p, partner, LEFT).start())

    def relay_corner(d, p):
        @pl.when(z == d)
        def _():
            moved(p, 1 - x, RIGHT).wait_recv()
            pl.when(has_right)(lambda: moved(p, 1 - x, RIGHT).start())

        @pl.when(z + d == line - 1)
        def _():
            origin = 2 * (line - 1) + 1 - x
            moved(p, origin, LEFT).wait_recv()
            pl.when(has_left)(lambda: moved(p, origin, LEFT).start())

    key_id = lax.broadcasted_iota(jnp.int32, (tok, 1), 0).astype(f32)
    dec_lane = lax.broadcasted_iota(jnp.int32, (1, dec_lanes), 1)
    small_copies[0].wait()
    dec_limit = jnp.zeros((1, dec_lanes), jnp.int32)
    for i in range(n_dec):
        dec_limit = jnp.where(
            jnp.logical_and(dec_lane % n_dec == i, dec_lane < GROUP * n_dec), pos_ref[i], dec_limit
        )
    dec_limit = dec_limit.astype(f32)
    query_row = (lax.broadcasted_iota(jnp.int32, (1, rows), 1) % tok).astype(f32)

    def weigh(block, h, diagonal=False):
        offset = own_off if diagonal else kbuf[block, 0, pl.ds(tok, MARK), :][0:1, 0:1].astype(f32)
        scores = lax.dot_general(
            kbuf[block, h, pl.ds(0, tok), :], qs[h], (((1,), (1,)), ((), ())),
            preferred_element_type=f32,
        )
        dec_seen = offset * tok + key_id < dec_limit
        dec_scores = jnp.where(dec_seen, scores[:, rows:], masked_score)
        scores = scores[:, :rows]
        if diagonal:
            scores = jnp.where(key_id <= query_row, scores, masked_score)
        old = m_ref[h][0:1]
        top = jnp.max(scores, axis=0, keepdims=True)
        new = jnp.maximum(old[:, :rows], top)
        if diagonal:
            used = new
        else:
            seen = offset <= own_off
            new = jnp.where(seen, new, old[:, :rows])
            used = jnp.where(seen, new, -masked_score)
        dec_new = jnp.maximum(old[:, rows:], jnp.max(dec_scores, axis=0, keepdims=True))
        new = jnp.concatenate([new, dec_new], axis=1)
        weights = jnp.concatenate([
            jnp.exp2((scores - used) * exp2_scale),
            jnp.exp2((dec_scores - dec_new) * exp2_scale),
        ], axis=1)
        factor = jnp.exp2((old - new) * exp2_scale)
        m_ref[h] = jnp.broadcast_to(new, m_ref.shape[1:])
        l_ref[h] = l_ref[h] * factor + jnp.sum(weights, axis=0, keepdims=True)
        return weights.astype(b16), factor

    def gather_values(block, h, weights, factor):
        added = lax.dot_general(
            vbuf[block, h], weights, (((0,), (0,)), ((), ())), preferred_element_type=f32
        )
        acc_ref[h] = acc_ref[h] * factor + added

    def attend(block, diagonal=False):
        weighed = [weigh(block, h, diagonal) for h in range(kv_heads)]
        for h in range(kv_heads):
            gather_values(block, h, *weighed[h])

    for copy in small_copies[1:]:
        copy.wait()
    pad = dec_lanes - GROUP * n_dec
    for h in range(kv_heads):
        q32 = jnp.concatenate([
            aq_ref[:, (h * GROUP + g) * HEAD_SIZE : (h * GROUP + g + 1) * HEAD_SIZE].astype(f32)
            for g in range(GROUP)
        ] + ([jnp.zeros((pad, HEAD_SIZE), f32)] if pad else []), axis=0)
        dec_q = q32.astype(b16)
        qs[h, pl.ds(rows, dec_lanes), :] = dec_q
        cols = slice(h * HEAD_SIZE, (h + 1) * HEAD_SIZE)
        own_lane = lax.broadcasted_iota(jnp.int32, (n_dec, dec_lanes), 1)
        own_token = lax.broadcasted_iota(jnp.int32, (n_dec, dec_lanes), 0)
        mine = jnp.logical_and(own_lane % n_dec == own_token, own_lane < GROUP * n_dec)
        pair_scores = lax.dot_general(
            ak_ref[:, cols], dec_q, (((1,), (1,)), ((), ())), preferred_element_type=f32
        )
        self_score = jnp.sum(jnp.where(mine, pair_scores, 0.0), axis=0, keepdims=True)
        picked = lax.dot_general(
            av_ref[:, cols].astype(f32), mine.astype(f32), (((0,), (0,)), ((), ())),
            preferred_element_type=f32,
        )
        m_ref[h] = jnp.broadcast_to(
            jnp.concatenate([jnp.full((1, rows), masked_score, f32), self_score], axis=1),
            m_ref.shape[1:],
        )
        l_ref[h] = jnp.concatenate(
            [jnp.zeros((8, rows), f32), jnp.ones((8, dec_lanes), f32)], axis=1
        )
        acc_ref[h] = jnp.concatenate([jnp.zeros((HEAD_SIZE, rows), f32), picked], axis=1)
    for copy in q_copies:
        copy.wait()
    attend(seq, diagonal=True)

    edge = jnp.logical_or(z == 0, z == line - 1)

    def near(d):
        pl.when(z >= d)(lambda: attend(2 * (z - d) + x))
        pl.when(z + d < line)(lambda: attend(2 * (z + d) + x))

    def await_side(d, h):
        for p in (2 * h, 2 * h + 1):
            if h == early_head:
                pl.when(z > d)(lambda: moved(p, 2 * (z - d) + 1 - x, SIDE).wait_recv())
                pl.when(z + d < line - 1)(
                    lambda: moved(p, 2 * (z + d) + 1 - x, SIDE).wait_recv()
                )
            else:
                pl.when(z >= d)(lambda: moved(p, 2 * (z - d) + 1 - x, SIDE).wait_recv())
                pl.when(z + d < line)(lambda: moved(p, 2 * (z + d) + 1 - x, SIDE).wait_recv())

    def across(d):
        for h in range(kv_heads):
            await_side(d, h)
        pl.when(z >= d)(lambda: attend(2 * (z - d) + 1 - x))
        pl.when(z + d < line)(lambda: attend(2 * (z + d) + 1 - x))

    corner_k, corner_v = 2 * early_head, 2 * early_head + 1

    for p in range(len(pieces)):
        relay_own(1, p)
        relay_partner(sideways[p])
    near(1)

    def round_(r, carry):
        for p in range(len(pieces)):
            relay_own(r, p)
            if p == 1:
                relay_corner(r - 1, corner_k)
                pl.when(both(r == 2, edge))(lambda: attend(partner))
                pl.when(both(r > 2, edge))(lambda: across(r - 2))
            if p == 2:
                relay_corner(r - 1, corner_v)
        near(r)
        pl.when(both(r == 2, jnp.logical_not(edge)))(lambda: attend(partner))
        pl.when(both(r > 2, jnp.logical_not(edge)))(lambda: across(r - 2))
        return carry

    lax.fori_loop(2, line, round_, 0)
    across(line - 2)

    def finish(origin):
        for h in range(kv_heads - 1):
            moved(2 * h, origin, SIDE).wait_recv()
        relay_corner(line - 1, corner_k)
        weighed = [weigh(origin, h) for h in range(kv_heads)]
        for h in range(kv_heads - 1):
            moved(2 * h + 1, origin, SIDE).wait_recv()
        relay_corner(line - 1, corner_v)
        for h in range(kv_heads):
            gather_values(origin, h, *weighed[h])

    pl.when(z == line - 1)(lambda: finish(1 - x))
    pl.when(z == 0)(lambda: finish(2 * (line - 1) + 1 - x))

    dec_pad = attn.shape[0] - tok - n_dec
    for h in range(kv_heads):
        turned = jnp.transpose(acc_ref[h] * (1.0 / l_ref[h][0:1]))
        for g in range(GROUP):
            i = h * GROUP + g
            cols = slice(i * HEAD_SIZE, (i + 1) * HEAD_SIZE)
            attn[0:tok, cols] = turned[g * tok : (g + 1) * tok].astype(b16)
            dec = turned[rows + g * n_dec : rows + (g + 1) * n_dec]
            if dec_pad:
                dec = jnp.concatenate([dec, jnp.zeros((dec_pad, HEAD_SIZE), f32)], axis=0)
            attn[tok:, cols] = dec.astype(b16)
    weight_copy.wait()

    direct = xown.shape[1]
    n_chunk = (model - direct) // chunk
    ahead = 2

    def core_copy(i):
        return pltpu.make_async_remote_copy(
            src_ref=send1.at[i], dst_ref=recv1.at[i], send_sem=ss1.at[i], recv_sem=rs1.at[i],
            device_id=to_core, device_id_type=MESH,
        )

    def y_copy(i):
        return pltpu.make_async_remote_copy(
            src_ref=send2.at[i], dst_ref=recv2.at[i], send_sem=ss2.at[i], recv_sem=rs2.at[i],
            device_id=to_y, device_id_type=MESH,
        )

    def block(index):
        return pl.ds(pl.multiple_of(index * part, 8), part)

    def columns(i):
        return pl.ds(pl.multiple_of(direct + i * chunk, LANES), chunk)

    first = slice(0, direct)
    pbuf[:, first] = jnp.dot(attn[...], wbuf[:, first], preferred_element_type=f32)
    first_copies = []
    for way, (peer, owner) in enumerate((
        (to_y, 2 * (1 - y) + c), (to_diag, 2 * (1 - y) + 1 - c), (to_core, 2 * y + 1 - c),
    )):
        xsend[way] = pbuf[block(owner), first].astype(b16)
        first_copies.append(pltpu.make_async_remote_copy(
            src_ref=xsend.at[way], dst_ref=xrecv.at[way],
            send_sem=xss.at[way], recv_sem=xrs.at[way],
            device_id=peer, device_id_type=MESH,
        ))
        first_copies[-1].start()
    xown[...] = pbuf[block(2 * y + c), first]
    dpart[:, first] = pbuf[tok : tok + n_dec, first]

    def pass_on(i):
        core_copy(i).wait_recv()
        total = own[i, 0:part] + recv1[i, 0:part].astype(f32)
        send2[i] = total.astype(b16)
        y_copy(i).start()

    def project(i, carry):
        cols = columns(i)
        pbuf[:, 0:chunk] = jnp.dot(attn[...], wbuf[:, cols], preferred_element_type=f32)
        send1[i, 0:part] = pbuf[block(2 * (1 - y) + 1 - c), 0:chunk].astype(b16)
        send1[i, part:] = pbuf[block(2 * y + 1 - c), 0:chunk].astype(b16)
        core_copy(i).start()
        own[i, 0:part] = pbuf[block(2 * (1 - y) + c), 0:chunk]
        own[i, part:] = pbuf[block(2 * y + c), 0:chunk]
        dpart[:, cols] = pbuf[tok : tok + n_dec, 0:chunk]
        pl.when(i >= ahead)(lambda: pass_on(i - ahead))
        return carry

    lax.fori_loop(0, n_chunk, project, 0)

    quarter = model // 4
    mine = pl.ds(seq * own_dec, own_dec)

    def dec_copy(way, peer):
        return pltpu.make_async_remote_copy(
            src_ref=dsend.at[way], dst_ref=drecv.at[way],
            send_sem=dss.at[way], recv_sem=drs.at[way],
            device_id=peer, device_id_type=MESH,
        )

    dec_copies = []
    for way, peer in enumerate((to_core, to_y, to_diag)):
        cols = pl.ds(pl.multiple_of(peer[1] * quarter, 128), quarter)
        dsend[way] = dpart[mine, cols]
        dec_copies.append(dec_copy(way, peer))
        dec_copies[-1].start()

    for i in range(n_chunk - ahead, n_chunk):
        pass_on(i)

    def drain(oz, carry):
        origin = 2 * oz + x
        edge = jnp.logical_or(oz == 0, oz == line - 1)
        for p in range(len(pieces)):
            pl.when(both(oz <= z, has_right))(lambda: moved(p, origin, RIGHT).wait_send())
            pl.when(both(oz >= z, has_left))(lambda: moved(p, origin, LEFT).wait_send())
            if early(p):
                pl.when(jnp.logical_or(oz == z, jnp.logical_not(edge)))(
                    lambda: moved(p, origin, SIDE).wait_send()
                )
            else:
                moved(p, origin, SIDE).wait_send()
        return carry

    lax.fori_loop(0, line, drain, 0)
    for p in (corner_k, corner_v):
        pl.when(has_right)(lambda: moved(p, 1 - x, RIGHT).wait_send())
        pl.when(has_left)(lambda: moved(p, 2 * (line - 1) + 1 - x, LEFT).wait_send())

    def gather_sum(i, carry):
        y_copy(i).wait_recv()
        cols = columns(i)
        total = own[i, part:] + recv1[i, part:].astype(f32)
        out_ref[:, cols] = (total + recv2[i].astype(f32)).astype(b16)
        y_copy(i).wait_send()
        core_copy(i).wait_send()
        return carry

    for copy in first_copies:
        copy.wait()
    total = xown[...]
    for way in range(3):
        total = total + xrecv[way].astype(f32)
    out_ref[:, first] = total.astype(b16)
    lax.fori_loop(0, n_chunk - 1, gather_sum, 0)
    for copy in dec_copies:
        copy.wait()
    dec_total = dpart[mine, pl.ds(pl.multiple_of(head * quarter, 128), quarter)]
    dec_total = dec_total + drecv[0] + drecv[1] + drecv[2]
    dec_ref[...] = jnp.broadcast_to(dec_total, dec_ref.shape)
    gather_sum(n_chunk - 1, 0)


def on_device(
    prompt_queries, prompt_keys, prompt_values, span_offset,
    appended_queries, appended_keys, appended_values, dec_pos, out_weight,
):
    n_seq = lax.axis_size("seq")
    tok, width = prompt_queries.shape
    kv_width = prompt_keys.shape[1]
    kv_heads = kv_width // HEAD_SIZE
    heads = kv_heads * GROUP
    n_dec = appended_queries.shape[0]
    own_dec = n_dec // n_seq
    model = out_weight.shape[1]
    direct = 4 * LANES
    chunk = next(c for c in (512, 384, 256, LANES) if (model - direct) % c == 0)
    n_chunk = (model - direct) // chunk
    part = tok // 4
    rows = tok + -(-n_dec // 16) * 16
    lanes = GROUP * tok + -(-GROUP * n_dec // LANES) * LANES
    vmem = pl.BlockSpec(memory_space=pltpu.VMEM)
    hbm = pl.BlockSpec(memory_space=pltpu.MemorySpace.HBM)
    smem = pl.BlockSpec(memory_space=pltpu.SMEM)
    f32, b16 = jnp.float32, jnp.bfloat16
    dma = pltpu.SemaphoreType.DMA
    n_piece = 2 * kv_heads
    results = pl.pallas_call(
        functools.partial(kernel, n_seq, own_dec, chunk, n_dec, tok),
        out_shape=(
            jax.ShapeDtypeStruct((part, model), b16),
            jax.ShapeDtypeStruct((8 * own_dec, model // 4), f32),
        ),
        in_specs=[hbm] * 3 + [smem] + [hbm] * 5,
        out_specs=(vmem, vmem),
        scratch_shapes=[
            pltpu.VMEM((n_seq, kv_heads, tok + MARK, HEAD_SIZE), b16),
            pltpu.VMEM((n_seq, kv_heads, tok, HEAD_SIZE), b16),
            pltpu.VMEM(out_weight.shape, b16),
            pltpu.VMEM((kv_heads, lanes, HEAD_SIZE), b16),
            pltpu.VMEM((n_dec, width), b16),
            pltpu.VMEM((n_dec, kv_width), b16),
            pltpu.VMEM((n_dec, kv_width), b16),
            pltpu.VMEM((kv_heads, 8, lanes), f32),
            pltpu.VMEM((kv_heads, 8, lanes), f32),
            pltpu.VMEM((kv_heads, HEAD_SIZE, lanes), f32),
            pltpu.SMEM((n_dec,), jnp.int32),
            pltpu.VMEM((rows, width), b16),
            pltpu.VMEM((rows, max(chunk, direct)), f32),
            pltpu.VMEM((n_chunk, 2 * part, chunk), f32),
            pltpu.VMEM((n_chunk, 2 * part, chunk), b16),
            pltpu.VMEM((n_chunk, 2 * part, chunk), b16),
            pltpu.VMEM((n_chunk, part, chunk), b16),
            pltpu.VMEM((n_chunk, part, chunk), b16),
            pltpu.VMEM((part, direct), f32),
            pltpu.VMEM((3, part, direct), b16),
            pltpu.VMEM((3, part, direct), b16),
            pltpu.VMEM((n_dec, model), f32),
            pltpu.VMEM((3, own_dec, model // 4), f32),
            pltpu.VMEM((3, own_dec, model // 4), f32),
            dma((n_piece,)), dma((heads,)), dma((4,)), dma,
            dma((3, n_piece, n_seq)), dma((n_piece, n_seq)),
            dma((n_chunk,)), dma((n_chunk,)), dma((n_chunk,)), dma((n_chunk,)),
            dma((3,)), dma((3,)), dma((3,)), dma((3,)),
        ],
        compiler_params=pltpu.CompilerParams(
            collective_id=0, has_side_effects=True, vmem_limit_bytes=44 * 2**20
        ),
    )(
        *map(in_hbm, (prompt_queries, prompt_keys, prompt_values)), span_offset,
        *map(in_hbm, (appended_queries, appended_keys, appended_values, dec_pos, out_weight)),
    )
    return pl.pallas_call(
        hand_on,
        out_shape=(
            jax.ShapeDtypeStruct((part, model), b16),
            jax.ShapeDtypeStruct((own_dec, model // 4), b16),
        ),
        in_specs=[vmem] * 2,
        out_specs=(vmem, vmem),
        compiler_params=pltpu.CompilerParams(vmem_limit_bytes=4 * 2**20),
    )(*results)


def solution(mesh):
    in_specs = (
        P("seq", "head"),
        P("seq", "head"),
        P("seq", "head"),
        P("seq"),
        P(None, "head"),
        P(None, "head"),
        P(None, "head"),
        P(),
        P("head", None),
    )
    out_specs = (P(("seq", "head"), None), P("seq", "head"))
    return jax.shard_map(
        on_device, mesh=mesh, in_specs=in_specs, out_specs=out_specs, check_vma=False
    )
```
